16 devices in a mesh: data: 2 (over z), expert: 8 (over y, x, core).
Axes of the slice: x: 2, y: 2, z: 2, core: 2. Of those that a mesh axis runs over, the one named last changes fastest.
Arguments:
- x_tokens: bfloat16 [1024, 1024], P(('data', 'expert')), parts along dimension 0
- y_mid: bfloat16 [1024, 1024], P(('data', 'expert')), parts along dimension 0
- dy_out: bfloat16 [1024, 1024], P(('data', 'expert')), parts along dimension 0
- experts_one: int32 [1024, 8], P(('data', 'expert')), parts along dimension 0
- gates_one: float32 [1024, 8], P(('data', 'expert')), parts along dimension 0
- slots_one: int32 [1024, 8], P(('data', 'expert')), parts along dimension 0
- experts_two: int32 [1024, 8], P(('data', 'expert')), parts along dimension 0
- gates_two: float32 [1024, 8], P(('data', 'expert')), parts along dimension 0
- slots_two: int32 [1024, 8], P(('data', 'expert')), parts along dimension 0
- w_gate_one: bfloat16 [32, 1024, 512], P('expert')
- w_up_one: bfloat16 [32, 1024, 512], P('expert')
- w_down_one: bfloat16 [32, 512, 1024], P('expert')
- w_gate_two: bfloat16 [32, 1024, 512], P('expert')
- w_up_two: bfloat16 [32, 1024, 512], P('expert')
- w_down_two: bfloat16 [32, 512, 1024], P('expert')
Outputs:
- output 1: bfloat16 [1024, 1024], P(('data', 'expert')), parts along dimension 0
- output 2: float32 [64, 1024, 512], P(('data', 'expert')), parts along dimension 0
- output 3: float32 [64, 1024, 512], P(('data', 'expert')), parts along dimension 0
- output 4: float32 [64, 512, 1024], P(('data', 'expert')), parts along dimension 0
- output 5: float32 [64, 1024, 512], P(('data', 'expert')), parts along dimension 0
- output 6: float32 [64, 1024, 512], P(('data', 'expert')), parts along dimension 0
- output 7: float32 [64, 512, 1024], P(('data', 'expert')), parts along dimension 0
There are 2 independent parts. The reference program is written for one: setup_inputs(seed, part) draws one part's arguments, and reference() takes and returns one part's arrays. A program takes and returns all parts, laid end to end along the dimension named above; an argument that names none is the same for every part.
All inputs are finite; a program needn't handle non-finite values.
Results may differ from the reference program's by a relative error of at most 0.01323.
Values are sent between devices in bfloat16 or wider.
A program may use at most 1 GiB of HBM per device.

```python
import jax
import jax.numpy as jnp
from jax import lax

MODEL_DIM = 1024
FFN_DIM = 512
EXPERTS = 32
TOP_K = 8
TOKENS_DEV = 64
GROUP_SIZE = 8

TOKENS_PART = GROUP_SIZE * TOKENS_DEV
CAPACITY = 8 * ((3 * TOP_K * TOKENS_DEV + 16 * EXPERTS - 1) // (16 * EXPERTS))
TOTAL_ROWS = GROUP_SIZE * EXPERTS * CAPACITY


def draw_routing(key):
    key_noise, key_bias, key_hot = jax.random.split(key, 3)
    noise_int = jax.random.randint(key_noise, (TOKENS_PART, EXPERTS), 0, 4096)
    expert_bias = jax.random.randint(key_bias, (EXPERTS,), 0, 512)
    hot_expert = jax.random.randint(key_hot, (), 0, EXPERTS)
    expert_ids = jnp.arange(EXPERTS, dtype=jnp.int32)
    local_tok = jnp.arange(TOKENS_PART, dtype=jnp.int32) % TOKENS_DEV
    boost_int = jnp.where((local_tok[:, None] < CAPACITY) & (expert_ids[None, :] == hot_expert), 8192, 0)
    score_int = (noise_int + expert_bias[None, :] + boost_int) * EXPERTS + expert_ids[None, :]
    top_vals, experts = lax.top_k(score_int, TOP_K)
    flat_ids = experts.reshape(GROUP_SIZE, TOKENS_DEV * TOP_K)
    onehot = (flat_ids[:, :, None] == expert_ids[None, None, :]).astype(jnp.int32)
    slot_rank = jnp.sum((jnp.cumsum(onehot, axis=1) - 1) * onehot, axis=2)
    slots = jnp.where(slot_rank < CAPACITY, slot_rank, -1).reshape(TOKENS_PART, TOP_K)
    return experts.astype(jnp.int32), slots.astype(jnp.int32)


def draw_weight(key, shape, fan_in):
    return (jax.random.normal(key, shape, jnp.float32) * fan_in ** -0.5).astype(jnp.bfloat16)


def setup_inputs(seed: int = 0, part: int = 0) -> dict:
    key_part = jax.random.fold_in(jax.random.key(seed), part)
    keys = jax.random.split(key_part, 7)
    shared = jax.random.split(jax.random.key(seed + 1), 6)
    tok_shape = (TOKENS_PART, MODEL_DIM)
    route_shape = (TOKENS_PART, TOP_K)
    up_shape = (EXPERTS, MODEL_DIM, FFN_DIM)
    down_shape = (EXPERTS, FFN_DIM, MODEL_DIM)
    gate_scale = TOP_K ** -0.5
    experts_one, slots_one = draw_routing(keys[3])
    experts_two, slots_two = draw_routing(keys[4])
    return {
        "x_tokens": jax.random.normal(keys[0], tok_shape, jnp.float32).astype(jnp.bfloat16),
        "y_mid": jax.random.normal(keys[1], tok_shape, jnp.float32).astype(jnp.bfloat16),
        "dy_out": jax.random.normal(keys[2], tok_shape, jnp.float32).astype(jnp.bfloat16),
        "experts_one": experts_one,
        "gates_one": jax.random.uniform(keys[5], route_shape, jnp.float32, 0.5, 1.5) * gate_scale,
        "slots_one": slots_one,
        "experts_two": experts_two,
        "gates_two": jax.random.uniform(keys[6], route_shape, jnp.float32, 0.5, 1.5) * gate_scale,
        "slots_two": slots_two,
        "w_gate_one": draw_weight(shared[0], up_shape, MODEL_DIM),
        "w_up_one": draw_weight(shared[1], up_shape, MODEL_DIM),
        "w_down_one": draw_weight(shared[2], down_shape, FFN_DIM),
        "w_gate_two": draw_weight(shared[3], up_shape, MODEL_DIM),
        "w_up_two": draw_weight(shared[4], up_shape, MODEL_DIM),
        "w_down_two": draw_weight(shared[5], down_shape, FFN_DIM),
    }


def expert_grads(operands):
    x_rows, z_rows, w_gate, w_up, w_down = operands
    gate_act = jnp.dot(x_rows, w_gate, preferred_element_type=jnp.float32).astype(jnp.bfloat16).astype(jnp.float32)
    up_act = jnp.dot(x_rows, w_up, preferred_element_type=jnp.float32).astype(jnp.bfloat16).astype(jnp.float32)
    sig_gate = jax.nn.sigmoid(gate_act)
    silu_gate = gate_act * sig_gate
    hidden = (silu_gate * up_act).astype(jnp.bfloat16)
    d_hidden = jnp.dot(z_rows, w_down.T, preferred_element_type=jnp.float32)
    dw_down = jnp.dot(hidden.T, z_rows, preferred_element_type=jnp.float32)
    d_gate = (d_hidden * up_act * sig_gate * (1.0 + gate_act * (1.0 - sig_gate))).astype(jnp.bfloat16)
    d_up = (d_hidden * silu_gate).astype(jnp.bfloat16)
    dx_rows = (jnp.dot(d_gate, w_gate.T, preferred_element_type=jnp.float32) + jnp.dot(d_up, w_up.T, preferred_element_type=jnp.float32)).astype(jnp.bfloat16)
    dw_gate = jnp.dot(x_rows.T, d_gate, preferred_element_type=jnp.float32)
    dw_up = jnp.dot(x_rows.T, d_up, preferred_element_type=jnp.float32)
    return dx_rows, dw_gate, dw_up, dw_down


def layer_backward(inputs, cotangent, experts, gates, slots, w_gate, w_up, w_down):
    source = jnp.arange(TOKENS_PART, dtype=jnp.int32) // TOKENS_DEV
    target = jnp.where(slots >= 0, (source[:, None] * EXPERTS + experts) * CAPACITY + slots, TOTAL_ROWS).reshape(-1)
    x_copies = jnp.repeat(inputs, TOP_K, axis=0)
    z_copies = (gates[:, :, None] * cotangent[:, None, :].astype(jnp.float32)).astype(jnp.bfloat16).reshape(TOKENS_PART * TOP_K, MODEL_DIM)
    x_buffer = jnp.zeros((TOTAL_ROWS + 1, MODEL_DIM), jnp.bfloat16).at[target].add(x_copies)
    z_buffer = jnp.zeros((TOTAL_ROWS + 1, MODEL_DIM), jnp.bfloat16).at[target].add(z_copies)
    by_source = (GROUP_SIZE, EXPERTS, CAPACITY, MODEL_DIM)
    by_expert = (EXPERTS, GROUP_SIZE * CAPACITY, MODEL_DIM)
    x_rows = x_buffer[:TOTAL_ROWS].reshape(by_source).transpose(1, 0, 2, 3).reshape(by_expert)
    z_rows = z_buffer[:TOTAL_ROWS].reshape(by_source).transpose(1, 0, 2, 3).reshape(by_expert)
    dx_rows, dw_gate, dw_up, dw_down = lax.map(expert_grads, (x_rows, z_rows, w_gate, w_up, w_down))
    returned = dx_rows.reshape(EXPERTS, GROUP_SIZE, CAPACITY, MODEL_DIM).transpose(1, 0, 2, 3).reshape(TOTAL_ROWS, MODEL_DIM)
    returned = jnp.concatenate([returned, jnp.zeros((1, MODEL_DIM), jnp.bfloat16)], axis=0)
    per_copy = returned[target].reshape(TOKENS_PART, TOP_K, MODEL_DIM).astype(jnp.float32)
    return jnp.sum(per_copy, axis=1), dw_gate, dw_up, dw_down


def reference(x_tokens, y_mid, dy_out, experts_one, gates_one, slots_one, experts_two, gates_two, slots_two, w_gate_one, w_up_one, w_down_one, w_gate_two, w_up_two, w_down_two):
    grads_two = layer_backward(y_mid, dy_out, experts_two, gates_two, slots_two, w_gate_two, w_up_two, w_down_two)
    dy_mid = (dy_out.astype(jnp.float32) + grads_two[0]).astype(jnp.bfloat16)
    grads_one = layer_backward(x_tokens, dy_mid, experts_one, gates_one, slots_one, w_gate_one, w_up_one, w_down_one)
    dx_tokens = (dy_mid.astype(jnp.float32) + grads_one[0]).astype(jnp.bfloat16)
    return (dx_tokens, grads_one[1], grads_one[2], grads_one[3], grads_two[1], grads_two[2], grads_two[3])
```

```python
import functools

import jax
import jax.numpy as jnp
from jax import lax
from jax.experimental import pallas as pl
from jax.experimental.pallas import tpu as pltpu
from jax.sharding import PartitionSpec as P

GROUP = 8
EXP = 4
CAP = 24
TOK = 64
DIM = 1024
FFN = 512
PAIR = 2 * CAP
ROWS = GROUP * CAP
NK = 4
KC = DIM // NK
BF = jnp.bfloat16
F32 = jnp.float32
NT = (((1,), (1,)), ((), ()))
TN = (((0,), (0,)), ((), ()))


def dot(a, b, dims=(((1,), (0,)), ((), ()))):
    return lax.dot_general(a, b, dims, preferred_element_type=F32)


def exchange_kernel(
    y_hbm, dy_hbm, x_hbm, e2, g2, s2, e1, g1, s1, wg2, wu2, wd2, wg1, wu1, wd1,
    u2_o, z2_o, h2_o, a2_o, b2_o, u1_o, z1_o, h1_o, a1_o, b1_o, t1a_o, t1b_o, t1c_o, t1d_o, dym_o,
    wg, wu, wd, tok, dmid, route, sel, gate, u, z, actA, actB, hid, dA, dB, dh, dxk, s_oth, s_rcv, s_own, rs_rcv,
    w_sem, l_sem, r_send, r_recv, g_send, g_recv, d_send, d_recv, c_send, c_recv, p_send, p_recv, o_sem,
):
    me = lax.axis_index("expert")
    core = lax.rem(me, 2)
    bx = lax.rem(me // 2, 2)
    by = me // 4
    partner = me + 1 - 2 * core
    devs = (None, me + 2 - 4 * bx, me + 4 - 8 * by, me + 6 - 4 * bx - 8 * by)

    def remote(src, dst, ss, rs, dev):
        return pltpu.make_async_remote_copy(
            src_ref=src, dst_ref=dst, send_sem=ss, recv_sem=rs, device_id={"expert": dev}, device_id_type=pl.DeviceIdType.MESH
        )

    local = [pltpu.make_async_copy(src, tok.at[a, 0], l_sem.at[a]) for a, src in enumerate((y_hbm, dy_hbm, x_hbm))]
    for c in local:
        c.start()
    wcopies = []
    for n, (src, dst) in enumerate(((wg2, wg.at[1]), (wu2, wu.at[1]), (wd2, wd.at[1]), (wg1, wg.at[0]), (wu1, wu.at[0]), (wd1, wd.at[0]))):
        wcopies.append(pltpu.make_async_copy(src, dst, w_sem.at[n]))

    def doubled(v):
        return jnp.concatenate([v, v], axis=1)

    for lay, (e, g, s) in enumerate(((e1, g1, s1), (e2, g2, s2))):
        code = jnp.where(s[...] >= 0, e[...] * PAIR + s[...], -1000000).astype(F32)
        route[0, 2 * lay] = doubled(code)
        route[0, 2 * lay + 1] = doubled(g[...])

    barrier = pltpu.get_barrier_semaphore()
    for dev in (partner,) + devs[1:]:
        pl.semaphore_signal(barrier, inc=1, device_id={"expert": dev}, device_id_type=pl.DeviceIdType.MESH)
    pl.semaphore_wait(barrier, 4)

    def gather(view, send, recv):
        direct = [remote(view(0), view(2 * p), send.at[p], recv.at[2 * p], devs[p]) for p in (1, 2, 3)]
        own = remote(view(0), view(1), send.at[0], recv.at[1], partner)
        fwd = [remote(view(2 * p), view(2 * p + 1), send.at[3 + p], recv.at[2 * p + 1], partner) for p in (1, 2, 3)]
        return direct, own, fwd

    def launch(g):
        for c in g[0]:
            c.start()
        g[1].start()

    def forward(g):
        for c, f in zip(g[0], g[2]):
            c.wait_recv()
            f.start()

    rt = gather(lambda k: route.at[k], r_send, r_recv)
    tg = [gather(lambda k, a=a: tok.at[a, k], g_send.at[a], g_recv.at[a]) for a in range(3)]
    launch(rt)
    for a in range(3):
        local[a].wait()
        launch(tg[a])
    for c in wcopies:
        c.start()

    forward(rt)
    rt[1].wait_recv()
    for f in rt[2]:
        f.wait_recv()

    lane = lax.broadcasted_iota(jnp.int32, (8, 2 * TOK), 1)
    row = lax.broadcasted_iota(jnp.int32, (EXP * PAIR, 2 * TOK), 0).astype(F32)
    base = (me * (EXP * PAIR)).astype(F32)

    def build_select(lay):
        for p in range(4):
            code = jnp.where(lane < TOK, route[2 * p, 2 * lay], route[2 * p + 1, 2 * lay] + CAP) - base
            gates = jnp.where(lane < TOK, route[2 * p, 2 * lay + 1], route[2 * p + 1, 2 * lay + 1])
            hit = jnp.zeros((EXP * PAIR, 2 * TOK), F32)
            total = jnp.zeros((EXP * PAIR, 2 * TOK), F32)
            for j in range(8):
                match = row == code[j : j + 1, :]
                hit = jnp.where(match, 1.0, hit)
                total = jnp.where(match, gates[j : j + 1, :], total)
            sel[lay, p] = hit.astype(BF)
            gate[lay, p] = jnp.broadcast_to(jnp.sum(total, axis=1, keepdims=True), (EXP * PAIR, 128))

    build_select(1)

    def put_rows(dst, p, cols, rows):
        for e in range(EXP):
            dst[e, p * PAIR : (p + 1) * PAIR, cols] = rows[e * PAIR : (e + 1) * PAIR, :]

    def pick_rows(lay, p, block):
        return dot(sel[lay, p], block)

    def build_u(lay, a, p):
        for k in range(NK):
            cols = slice(k * KC, (k + 1) * KC)
            block = jnp.concatenate([tok[a, 2 * p, :, cols], tok[a, 2 * p + 1, :, cols]], axis=0)
            put_rows(u.at[lay], p, cols, pick_rows(lay, p, block).astype(BF))

    def build_z(lay, p, cols, first, second):
        rows = pick_rows(lay, p, jnp.concatenate([first, second], axis=0))
        g = gate[lay, p]
        rows = jnp.concatenate([rows[:, i * 128 : (i + 1) * 128] * g for i in range(KC // 128)], axis=1)
        put_rows(z.at[lay], p, cols, rows.astype(BF))

    def recompute(lay):
        def body(e, _):
            actA[lay, e] = dot(u[lay, e], wg[lay, e]).astype(BF)
            actB[lay, e] = dot(u[lay, e], wu[lay, e]).astype(BF)
            return 0

        lax.fori_loop(0, EXP, body, 0)

    def activation_grads(lay, e, d_hid):
        a = actA[lay, e].astype(F32)
        b = actB[lay, e].astype(F32)
        sig = jax.nn.sigmoid(a)
        silu = a * sig
        hid[lay, e] = (silu * b).astype(BF)
        dA[lay, e] = (d_hid * b * sig * (1.0 + a * (1.0 - sig))).astype(BF)
        dB[lay, e] = (d_hid * silu).astype(BF)

    def return_rows(lay, k):
        def body(e, _):
            cols = slice(k * KC, (k + 1) * KC)
            rows = dot(dA[lay, e], wg[lay, e, cols, :], NT) + dot(dB[lay, e], wu[lay, e, cols, :], NT)
            rows = rows.astype(BF)
            for p in range(4):
                dxk[p, e] = rows[p * PAIR : (p + 1) * PAIR, :]
            return 0

        lax.fori_loop(0, EXP, body, 0)
        for p in range(4):
            part = dot(sel[lay, p], dxk[p].reshape(EXP * PAIR, KC), TN)
            s_own[lay, k, p] = part[:TOK, :]
            s_oth[lay, k, p] = part[TOK:, :]

    chip = [
        [remote(s_oth.at[lay, k], s_rcv.at[lay, k], c_send.at[lay, k], c_recv.at[lay, k], partner) for k in range(NK)]
        for lay in range(2)
    ]
    scatter = [
        [remote(s_own.at[1, k, p], rs_rcv.at[k, p], p_send.at[k, p], p_recv.at[k, p], devs[p]) for p in (1, 2, 3)]
        for k in range(NK)
    ]

    forward(tg[0])
    tg[0][1].wait_recv()
    for f in tg[0][2]:
        f.wait_recv()
    for p in range(4):
        build_u(1, 0, p)
    wcopies[0].wait()
    wcopies[1].wait()
    recompute(1)
    forward(tg[1])
    build_select(0)
    tg[1][1].wait_recv()
    for f in tg[1][2]:
        f.wait_recv()
    for p in range(4):
        for k in range(NK):
            cols = slice(k * KC, (k + 1) * KC)
            build_z(1, p, cols, tok[1, 2 * p, :, cols], tok[1, 2 * p + 1, :, cols])
    wcopies[2].wait()

    def body2(e, _):
        activation_grads(1, e, dot(z[1, e], wd[1, e], NT))
        return 0

    lax.fori_loop(0, EXP, body2, 0)

    outs = []

    def save(n, src, dst):
        c = pltpu.make_async_copy(src, dst, o_sem.at[n])
        c.start()
        outs.append(c)

    save(0, u.at[1], u2_o)
    save(1, z.at[1], z2_o)
    save(2, hid.at[1], h2_o)
    save(3, dA.at[1], a2_o)
    save(4, dB.at[1], b2_o)

    def combine(lay, k):
        chip[lay][k].wait_recv()
        for p in range(4):
            s_own[lay, k, p] = s_own[lay, k, p] + s_rcv[lay, k, p]

    for k in range(NK):
        return_rows(1, k)
        chip[1][k].start()
        if k:
            combine(1, k - 1)
            for c in scatter[k - 1]:
                c.start()
    combine(1, NK - 1)
    for c in scatter[NK - 1]:
        c.start()

    forward(tg[2])
    tg[2][1].wait_recv()
    for f in tg[2][2]:
        f.wait_recv()
    for p in range(4):
        build_u(0, 2, p)
    save(5, u.at[0], u1_o)
    wcopies[3].wait()
    wcopies[4].wait()
    recompute(0)

    mid = [gather(lambda s, k=k: dmid.at[k, s], d_send.at[k], d_recv.at[k]) for k in range(NK)]
    for k in range(NK):
        for c in scatter[k]:
            c.wait_recv()
        total = s_own[1, k, 0] + rs_rcv[k, 1] + rs_rcv[k, 2] + rs_rcv[k, 3]
        dmid[k, 0] = (tok[1, 0, :, k * KC : (k + 1) * KC].astype(F32) + total).astype(BF)
        launch(mid[k])
    wcopies[5].wait()

    def middle(k):
        mid[k][1].wait_recv()
        for f in mid[k][2]:
            f.wait_recv()
        cols = slice(k * KC, (k + 1) * KC)
        for p in range(4):
            build_z(0, p, cols, dmid[k, 2 * p], dmid[k, 2 * p + 1])

        def body(e, _):
            part = dot(z[0, e, :, cols], wd[0, e, :, cols], NT)
            dh[e] = part if k == 0 else dh[e] + part
            return 0

        lax.fori_loop(0, EXP, body, 0)

    for k in range(NK):
        forward(mid[k])
        if k:
            middle(k - 1)
    for k in range(NK):
        dym_c = pltpu.make_async_copy(dmid.at[k, 0], dym_o.at[:, pl.ds(k * KC, KC)], o_sem.at[12 + k])
        dym_c.start()
        outs.append(dym_c)
    middle(NK - 1)
    save(6, z.at[0], z1_o)

    def body1(e, _):
        activation_grads(0, e, dh[e])
        return 0

    lax.fori_loop(0, EXP, body1, 0)
    save(7, hid.at[0], h1_o)
    save(8, dA.at[0], a1_o)
    save(9, dB.at[0], b1_o)

    def finish(k):
        combine(0, k)
        for p, t1_o in enumerate((t1a_o, t1b_o, t1c_o, t1d_o)):
            c = pltpu.make_async_copy(s_own.at[0, k, p], t1_o.at[:, pl.ds(k * KC, KC)], o_sem.at[16 + 4 * k + p])
            c.start()
            outs.append(c)

    for k in range(NK):
        return_rows(0, k)
        chip[0][k].start()
        if k:
            finish(k - 1)
    finish(NK - 1)

    for g in [rt] + tg + mid:
        for c in g[0] + [g[1]] + g[2]:
            c.wait_send()
    for lay in range(2):
        for c in chip[lay]:
            c.wait_send()
    for cs in scatter:
        for c in cs:
            c.wait_send()
    for c in outs:
        c.wait()


def exchange(*args):
    rows = lambda n: jax.ShapeDtypeStruct((EXP, ROWS, n), BF)
    per_layer = [rows(DIM), rows(DIM), rows(FFN), rows(FFN), rows(FFN)]
    any_spec = pl.BlockSpec(memory_space=pl.ANY)
    vmem_spec = pl.BlockSpec(memory_space=pltpu.VMEM)
    dma = pltpu.SemaphoreType.DMA
    return pl.pallas_call(
        exchange_kernel,
        out_shape=per_layer + per_layer + [jax.ShapeDtypeStruct((TOK, DIM), F32)] * 4 + [jax.ShapeDtypeStruct((TOK, DIM), BF)],
        in_specs=[any_spec] * 3 + [vmem_spec] * 6 + [any_spec] * 6,
        out_specs=[any_spec] * 15,
        scratch_shapes=[
            pltpu.VMEM((2, EXP, DIM, FFN), BF),
            pltpu.VMEM((2, EXP, DIM, FFN), BF),
            pltpu.VMEM((2, EXP, FFN, DIM), BF),
            pltpu.VMEM((3, GROUP, TOK, DIM), BF),
            pltpu.VMEM((NK, GROUP, TOK, KC), BF),
            pltpu.VMEM((GROUP, 4, 8, 2 * TOK), F32),
            pltpu.VMEM((2, 4, EXP * PAIR, 2 * TOK), BF),
            pltpu.VMEM((2, 4, EXP * PAIR, 128), F32),
            pltpu.VMEM((2, EXP, ROWS, DIM), BF),
            pltpu.VMEM((2, EXP, ROWS, DIM), BF),
            pltpu.VMEM((2, EXP, ROWS, FFN), BF),
            pltpu.VMEM((2, EXP, ROWS, FFN), BF),
            pltpu.VMEM((2, EXP, ROWS, FFN), BF),
            pltpu.VMEM((2, EXP, ROWS, FFN), BF),
            pltpu.VMEM((2, EXP, ROWS, FFN), BF),
            pltpu.VMEM((EXP, ROWS, FFN), F32),
            pltpu.VMEM((4, EXP, PAIR, KC), BF),
            pltpu.VMEM((2, NK, 4, TOK, KC), F32),
            pltpu.VMEM((2, NK, 4, TOK, KC), F32),
            pltpu.VMEM((2, NK, 4, TOK, KC), F32),
            pltpu.VMEM((NK, 4, TOK, KC), F32),
            dma((6,)),
            dma((3,)),
            dma((7,)),
            dma((8,)),
            dma((3, 7)),
            dma((3, 8)),
            dma((NK, 7)),
            dma((NK, 8)),
            dma((2, NK)),
            dma((2, NK)),
            dma((NK, 4)),
            dma((NK, 4)),
            dma((32,)),
        ],
        compiler_params=pltpu.CompilerParams(collective_id=0, has_side_effects=True, vmem_limit_bytes=60 * 2**20),
        cost_estimate=pl.CostEstimate(flops=10**10, bytes_accessed=40 * 2**20, transcendentals=0),
    )(*args)


def weight_grad_kernel(u2, z2, h2, a2, b2, u1, z1, h1, a1, b1, g2, p2, d2, g1, p1, d1):
    step = pl.program_id(0)

    def layer(u, z, h, a, b, g_o, p_o, d_o):
        g_o[0] = dot(u[0], a[0], TN)
        p_o[0] = dot(u[0], b[0], TN)
        d_o[0] = dot(h[0], z[0], TN)

    @pl.when(step < 8)
    def _():
        layer(u2, z2, h2, a2, b2, g2, p2, d2)

    @pl.when(step >= 8)
    def _():
        layer(u1, z1, h1, a1, b1, g1, p1, d1)


def weight_grads(*rows):
    def at(lay, split):
        def index(s):
            t = jnp.clip(s - 8 * lay, 0, 7)
            return (t // 2,) + ((0, t % 2) if split == "cols" else (t % 2, 0) if split == "rows" else (0, 0))

        return index

    half_d, half_f = DIM // 2, FFN // 2
    ins, outs, shapes = [], [], []
    for lay in range(2):
        ins += [
            pl.BlockSpec((1, ROWS, half_d), at(lay, "cols")),
            pl.BlockSpec((1, ROWS, DIM), at(lay, "")),
            pl.BlockSpec((1, ROWS, half_f), at(lay, "cols")),
            pl.BlockSpec((1, ROWS, FFN), at(lay, "")),
            pl.BlockSpec((1, ROWS, FFN), at(lay, "")),
        ]
        outs += [pl.BlockSpec((1, half_d, FFN), at(lay, "rows"))] * 2 + [pl.BlockSpec((1, half_f, DIM), at(lay, "rows"))]
        up = jax.ShapeDtypeStruct((EXP, DIM, FFN), F32)
        shapes += [up, up, jax.ShapeDtypeStruct((EXP, FFN, DIM), F32)]
    return pl.pallas_call(
        weight_grad_kernel,
        grid=(16,),
        in_specs=ins,
        out_specs=outs,
        out_shape=shapes,
        compiler_params=pltpu.CompilerParams(vmem_limit_bytes=60 * 2**20),
        cost_estimate=pl.CostEstimate(flops=6 * 10**9, bytes_accessed=62 * 2**20, transcendentals=0),
    )(*rows)


def solution(mesh):
    tok_spec = P(("data", "expert"), None)
    weight_spec = P("expert", None, None)
    grad_spec = P(("data", "expert"), None, None)

    def local_step(x_tokens, y_mid, dy_out, experts_one, gates_one, slots_one, experts_two, gates_two, slots_two, w_gate_one, w_up_one, w_down_one, w_gate_two, w_up_two, w_down_two):
        res = exchange(
            y_mid, dy_out, x_tokens, experts_two.T, gates_two.T, slots_two.T, experts_one.T, gates_one.T, slots_one.T,
            w_gate_two, w_up_two, w_down_two, w_gate_one, w_up_one, w_down_one,
        )
        part, mid = res[10:14], res[14]
        back = [lax.ppermute(part[p], "expert", [(i, i ^ (2 * p)) for i in range(GROUP)]) for p in (1, 2, 3)]
        grads = weight_grads(*res[:10])
        total = part[0] + back[0] + back[1] + back[2]
        dx = (mid.astype(F32) + total).astype(BF)
        return (dx, grads[3], grads[4], grads[5], grads[0], grads[1], grads[2])

    return jax.shard_map(local_step, mesh=mesh, in_specs=(tok_spec,) * 9 + (weight_spec,) * 6, out_specs=(tok_spec,) + (grad_spec,) * 6, check_vma=False)
```

```python
import functools

import jax
import jax.numpy as jnp
from jax import lax
from jax.experimental import pallas as pl
from jax.experimental.pallas import tpu as pltpu
from jax.sharding import PartitionSpec as P

GROUP = 8
EXP = 4
CAP = 24
TOK = 64
DIM = 1024
FFN = 512
PAIR = 2 * CAP
ROWS = GROUP * CAP
NK = 4
KC = DIM // NK
BF = jnp.bfloat16
F32 = jnp.float32
NT = (((1,), (1,)), ((), ()))
TN = (((0,), (0,)), ((), ()))


def dot(a, b, dims=(((1,), (0,)), ((), ()))):
    return lax.dot_general(a, b, dims, preferred_element_type=F32)


class Copy:
    def __init__(self, copy, log):
        self.copy, self.log, self.arrived = copy, log, False

    def start(self):
        self.copy.start()
        self.log.append(self)

    def wait_recv(self):
        self.copy.wait_recv()
        self.arrived = True

    def drain(self):
        if not self.arrived:
            self.copy.wait_recv()
        self.copy.wait_send()


def exchange_kernel(
    y_hbm, dy_hbm, x_hbm, e2, g2, s2, e1, g1, s1, wg2, wu2, wd2, wg1, wu1, wd1,
    u2, z2, hid2, dab2, u1, z1, hid1, dab1, t1a, t1b, t1c, t1d, dym,
    wcat, wd, tok, dmid, raw_int, raw_gate, route, sel, selt, gate, act, dh, dx, s_oth, s_rcv, s_own, rs_rcv,
    w_sem, l_sem, r_send, r_recv, g_send, g_recv, d_send, d_recv, c_send, c_recv, p_send, p_recv,
):
    me = lax.axis_index("expert")
    core = lax.rem(me, 2)
    bx = lax.rem(me // 2, 2)
    by = me // 4
    partner = me + 1 - 2 * core
    devs = (None, me + 2 - 4 * bx, me + 4 - 8 * by, me + 6 - 4 * bx - 8 * by)
    u, z, hid, dab, t1 = (u1, u2), (z1, z2), (hid1, hid2), (dab1, dab2), (t1a, t1b, t1c, t1d)
    sent = []

    def remote(src, dst, ss, rs, dev):
        copy = pltpu.make_async_remote_copy(
            src_ref=src, dst_ref=dst, send_sem=ss, recv_sem=rs, device_id={"expert": dev}, device_id_type=pl.DeviceIdType.MESH
        )
        return Copy(copy, sent)

    local = [pltpu.make_async_copy(src, tok.at[a, 0], l_sem.at[a]) for a, src in enumerate((y_hbm, dy_hbm, x_hbm))]
    tables = ((e1, raw_int.at[0]), (s1, raw_int.at[1]), (g1, raw_gate.at[0]), (e2, raw_int.at[2]), (s2, raw_int.at[3]), (g2, raw_gate.at[1]))
    tables = [pltpu.make_async_copy(src, dst, l_sem.at[3 + n]) for n, (src, dst) in enumerate(tables)]
    for c in tables + local:
        c.start()
    left, right = pl.ds(0, FFN), pl.ds(FFN, FFN)
    weights = []
    for n, (src, dst) in enumerate(
        (
            (wg2, wcat.at[1, :, :, left]), (wu2, wcat.at[1, :, :, right]), (wd2, wd.at[1]),
            (wg1, wcat.at[0, :, :, left]), (wu1, wcat.at[0, :, :, right]), (wd1, wd.at[0]),
        )
    ):
        weights.append(pltpu.make_async_copy(src, dst, w_sem.at[n]))

    barrier = pltpu.get_barrier_semaphore()
    for dev in (partner,) + devs[1:]:
        pl.semaphore_signal(barrier, inc=1, device_id={"expert": dev}, device_id_type=pl.DeviceIdType.MESH)

    def doubled(v):
        return jnp.concatenate([v, v], axis=1)

    for c in tables:
        c.wait()
    for lay in range(2):
        experts, slots = raw_int[2 * lay], raw_int[2 * lay + 1]
        code = jnp.where(slots >= 0, experts * PAIR + slots, -1000000).astype(F32)
        route[0, 2 * lay] = doubled(code)
        route[0, 2 * lay + 1] = doubled(raw_gate[lay])

    pl.semaphore_wait(barrier, 4)

    class Gather:
        def __init__(self, view, send, recv):
            self.direct = {p: remote(view(0), view(2 * p), send.at[p], recv.at[2 * p], devs[p]) for p in (3, 1, 2)}
            self.own = remote(view(0), view(1), send.at[0], recv.at[1], partner)
            self.passed = {p: remote(view(2 * p), view(2 * p + 1), send.at[3 + p], recv.at[2 * p + 1], partner) for p in (3, 1, 2)}

        def launch(self):
            for c in self.direct.values():
                c.start()
            self.own.start()

        def forward(self):
            for p in (1, 2, 3):
                self.direct[p].wait_recv()
                self.passed[p].start()

        def rest(self):
            self.own.wait_recv()
            for p in (1, 2, 3):
                self.passed[p].wait_recv()

    routing = Gather(lambda k: route.at[k], r_send, r_recv)
    tokens = [Gather(lambda k, a=a: tok.at[a, k], g_send.at[a], g_recv.at[a]) for a in range(3)]
    routing.launch()
    for a in range(3):
        local[a].wait()
        tokens[a].launch()
    for c in weights:
        c.start()
    routing.forward()
    routing.rest()

    lane = lax.broadcasted_iota(jnp.int32, (8, 2 * TOK), 1)
    row = lax.broadcasted_iota(jnp.int32, (EXP * PAIR, 2 * TOK), 0).astype(F32)
    base = (me * (EXP * PAIR)).astype(F32)

    def build_select(lay):
        for p in range(4):
            code = jnp.where(lane < TOK, route[2 * p, 2 * lay], route[2 * p + 1, 2 * lay] + CAP) - base
            gates = jnp.where(lane < TOK, route[2 * p, 2 * lay + 1], route[2 * p + 1, 2 * lay + 1])
            hit = jnp.zeros((EXP * PAIR, 2 * TOK), F32)
            total = jnp.zeros((EXP * PAIR, 2 * TOK), F32)
            for j in range(8):
                match = row == code[j : j + 1, :]
                hit = jnp.where(match, 1.0, hit)
                total = jnp.where(match, gates[j : j + 1, :], total)
            sel[lay, p] = hit.astype(BF)
            selt[lay, p] = hit.T.astype(BF)
            gate[lay, p] = jnp.broadcast_to(jnp.sum(total, axis=1, keepdims=True), (EXP * PAIR, 128))

    build_select(1)
    build_select(0)

    def put_rows(dst, p, cols, rows):
        for e in range(EXP):
            dst[e, p * PAIR : (p + 1) * PAIR, cols] = rows[e * PAIR : (e + 1) * PAIR, :]

    def columns(k):
        return slice(k * KC, (k + 1) * KC)

    def build_u(lay, a, p):
        for k in range(NK):
            block = jnp.concatenate([tok[a, 2 * p, :, columns(k)], tok[a, 2 * p + 1, :, columns(k)]], axis=0)
            put_rows(u[lay], p, columns(k), dot(sel[lay, p], block).astype(BF))

    def build_z(lay, p, k, first, second):
        rows = dot(sel[lay, p], jnp.concatenate([first, second], axis=0))
        g = gate[lay, p]
        rows = jnp.concatenate([rows[:, i * 128 : (i + 1) * 128] * g for i in range(KC // 128)], axis=1)
        put_rows(z[lay], p, columns(k), rows.astype(BF))

    def recompute(lay):
        for e in range(EXP):
            act[e] = dot(u[lay][e], wcat[lay, e]).astype(BF)

    def expert_rows(lay, e, d_hid):
        a = act[e, :, :FFN].astype(F32)
        b = act[e, :, FFN:].astype(F32)
        sig = jax.nn.sigmoid(a)
        silu = a * sig
        hid[lay][e] = (silu * b).astype(BF)
        dab[lay][e, :, :FFN] = (d_hid * b * sig * (1.0 + a * (1.0 - sig))).astype(BF)
        dab[lay][e, :, FFN:] = (d_hid * silu).astype(BF)
        rows = dot(dab[lay][e], wcat[lay, e], NT).astype(BF)
        for p in range(4):
            dx[p, e] = rows[p * PAIR : (p + 1) * PAIR, :]

    def chip_partial(lay, k):
        for p in range(4):
            part = dot(selt[lay, p], dx[p, :, :, columns(k)].reshape(EXP * PAIR, KC))
            s_own[lay, k, p] = part[:TOK, :]
            s_oth[lay, k, p] = part[TOK:, :]

    chip = [
        [remote(s_oth.at[lay, k], s_rcv.at[lay, k], c_send.at[lay, k], c_recv.at[lay, k], partner) for k in range(NK)]
        for lay in range(2)
    ]
    scatter = [
        [remote(s_own.at[1, k, p], rs_rcv.at[k, p], p_send.at[k, p], p_recv.at[k, p], devs[p]) for p in (3, 1, 2)]
        for k in range(NK)
    ]

    tokens[0].forward()
    tokens[0].rest()
    for p in range(4):
        build_u(1, 0, p)
    weights[0].wait()
    weights[1].wait()
    recompute(1)
    tokens[1].forward()
    tokens[1].rest()
    for p in range(4):
        for k in range(NK):
            build_z(1, p, k, tok[1, 2 * p, :, columns(k)], tok[1, 2 * p + 1, :, columns(k)])
    weights[2].wait()
    for e in range(EXP):
        expert_rows(1, e, dot(z[1][e], wd[1, e], NT))
    for k in range(NK):
        chip_partial(1, k)
        chip[1][k].start()
    for k in range(NK):
        chip[1][k].wait_recv()
        for p in (3, 1, 2, 0):
            s_own[1, k, p] = s_own[1, k, p] + s_rcv[1, k, p]
        for c in scatter[k]:
            c.start()

    tokens[2].forward()
    tokens[2].rest()
    for p in range(4):
        build_u(0, 2, p)
    weights[3].wait()
    weights[4].wait()
    recompute(0)

    middle = [Gather(lambda s, k=k: dmid.at[k, s], d_send.at[k], d_recv.at[k]) for k in range(NK)]
    for k in range(NK):
        for c in scatter[k]:
            c.wait_recv()
        total = s_own[1, k, 0] + rs_rcv[k, 1] + rs_rcv[k, 2] + rs_rcv[k, 3]
        new = (tok[1, 0, :, columns(k)].astype(F32) + total).astype(BF)
        dmid[k, 0] = new
        dym[:, columns(k)] = new
        middle[k].launch()
    weights[5].wait()

    def hidden_grad(k):
        middle[k].rest()
        for p in range(4):
            build_z(0, p, k, dmid[k, 2 * p], dmid[k, 2 * p + 1])
        for e in range(EXP):
            part = dot(z[0][e, :, columns(k)], wd[0, e, :, columns(k)], NT)
            dh[e] = part if k == 0 else dh[e] + part

    for k in range(NK):
        middle[k].forward()
        if k:
            hidden_grad(k - 1)
    hidden_grad(NK - 1)
    for e in range(EXP):
        expert_rows(0, e, dh[e])
    for k in range(NK):
        chip_partial(0, k)
        chip[0][k].start()
    for k in range(NK):
        chip[0][k].wait_recv()
        for p in range(4):
            t1[p][:, columns(k)] = s_own[0, k, p] + s_rcv[0, k, p]
    for c in sent:
        c.drain()


def exchange(*args):
    rows = lambda n: pltpu.VMEM((EXP, ROWS, n), BF)
    per_layer = [rows(DIM), rows(DIM), rows(FFN), rows(2 * FFN)]
    hbm_spec = pl.BlockSpec(memory_space=pltpu.HBM)
    vmem_spec = pl.BlockSpec(memory_space=pltpu.VMEM)
    dma = pltpu.SemaphoreType.DMA
    return pl.pallas_call(
        exchange_kernel,
        out_shape=per_layer + per_layer + [pltpu.VMEM((TOK, DIM), F32)] * 4 + [pltpu.VMEM((TOK, DIM), BF)],
        in_specs=[hbm_spec] * 15,
        out_specs=[vmem_spec] * 13,
        scratch_shapes=[
            pltpu.VMEM((2, EXP, DIM, 2 * FFN), BF),
            pltpu.VMEM((2, EXP, FFN, DIM), BF),
            pltpu.VMEM((3, GROUP, TOK, DIM), BF),
            pltpu.VMEM((NK, GROUP, TOK, KC), BF),
            pltpu.VMEM((4, 8, TOK), jnp.int32),
            pltpu.VMEM((2, 8, TOK), F32),
            pltpu.VMEM((GROUP, 4, 8, 2 * TOK), F32),
            pltpu.VMEM((2, 4, EXP * PAIR, 2 * TOK), BF),
            pltpu.VMEM((2, 4, 2 * TOK, EXP * PAIR), BF),
            pltpu.VMEM((2, 4, EXP * PAIR, 128), F32),
            pltpu.VMEM((EXP, ROWS, 2 * FFN), BF),
            pltpu.VMEM((EXP, ROWS, FFN), F32),
            pltpu.VMEM((4, EXP, PAIR, DIM), BF),
            pltpu.VMEM((2, NK, 4, TOK, KC), F32),
            pltpu.VMEM((2, NK, 4, TOK, KC), F32),
            pltpu.VMEM((2, NK, 4, TOK, KC), F32),
            pltpu.VMEM((NK, 4, TOK, KC), F32),
            dma((6,)),
            dma((9,)),
            dma((7,)),
            dma((8,)),
            dma((3, 7)),
            dma((3, 8)),
            dma((NK, 7)),
            dma((NK, 8)),
            dma((2, NK)),
            dma((2, NK)),
            dma((NK, 4)),
            dma((NK, 4)),
        ],
        compiler_params=pltpu.CompilerParams(collective_id=0, has_side_effects=True, vmem_limit_bytes=K1_VMEM * 2**20),
        cost_estimate=pl.CostEstimate(flops=10**10, bytes_accessed=40 * 2**20, transcendentals=0),
    )(*[pltpu.with_memory_space_constraint(a, pltpu.HBM) for a in args])


K1_VMEM = 46
MB = 256
SLOTS = 5


def weight_grad_kernel(u2, z2, h2, ab2, u1, z1, h1, ab1, g2, p2, d2, g1, p1, d1, g_buf, p_buf, d_buf, sem):
    flying = {}
    step = 0
    for u, z, h, ab, g_o, p_o, d_o in ((u2, z2, h2, ab2, g2, p2, d2), (u1, z1, h1, ab1, g1, p1, d1)):
        for e in range(EXP):
            slot = step % SLOTS
            for c in flying.pop(step - SLOTS, []):
                c.wait()
            mine = flying.setdefault(step, [])

            def write(buf, out, m, n):
                part = pl.ds(m * MB, MB)
                c = pltpu.make_async_copy(buf.at[slot, part], out.at[e, part], sem.at[slot, n])
                c.start()
                mine.append(c)

            for m in range(DIM // MB):
                span = slice(m * MB, (m + 1) * MB)
                both = dot(u[e, :, span], ab[e], TN)
                g_buf[slot, span, :] = both[:, :FFN]
                p_buf[slot, span, :] = both[:, FFN:]
                write(g_buf, g_o, m, m)
                write(p_buf, p_o, m, DIM // MB + m)
            for m in range(FFN // MB):
                span = slice(m * MB, (m + 1) * MB)
                d_buf[slot, span, :] = dot(h[e, :, span], z[e], TN)
                write(d_buf, d_o, m, 2 * (DIM // MB) + m)
            step += 1
    for cs in flying.values():
        for c in cs:
            c.wait()


def weight_grads(*rows):
    up = jax.ShapeDtypeStruct((EXP, DIM, FFN), F32)
    shapes = [up, up, jax.ShapeDtypeStruct((EXP, FFN, DIM), F32)] * 2
    return pl.pallas_call(
        weight_grad_kernel,
        in_specs=[pl.BlockSpec(memory_space=pltpu.VMEM)] * 8,
        out_specs=[pl.BlockSpec(memory_space=pl.ANY)] * 6,
        out_shape=shapes,
        scratch_shapes=[
            pltpu.VMEM((SLOTS, DIM, FFN), F32),
            pltpu.VMEM((SLOTS, DIM, FFN), F32),
            pltpu.VMEM((SLOTS, FFN, DIM), F32),
            pltpu.SemaphoreType.DMA((SLOTS, 2 * (DIM // MB) + FFN // MB)),
        ],
        compiler_params=pltpu.CompilerParams(vmem_limit_bytes=K2_VMEM * 2**20),
        cost_estimate=pl.CostEstimate(flops=6 * 10**9, bytes_accessed=62 * 2**20, transcendentals=0),
    )(*[pltpu.with_memory_space_constraint(r, pltpu.VMEM) for r in rows])


K2_VMEM = 36


def solution(mesh):
    tok_spec = P(("data", "expert"), None)
    weight_spec = P("expert", None, None)
    grad_spec = P(("data", "expert"), None, None)

    def local_step(x_tokens, y_mid, dy_out, experts_one, gates_one, slots_one, experts_two, gates_two, slots_two, w_gate_one, w_up_one, w_down_one, w_gate_two, w_up_two, w_down_two):
        res = exchange(
            y_mid, dy_out, x_tokens, experts_two.T, gates_two.T, slots_two.T, experts_one.T, gates_one.T, slots_one.T,
            w_gate_two, w_up_two, w_down_two, w_gate_one, w_up_one, w_down_one,
        )
        part, mid = res[8:12], res[12]
        back = [lax.ppermute(part[p], "expert", [(i, i ^ (2 * p)) for i in range(GROUP)]) for p in (1, 2, 3)]
        grads = weight_grads(*res[:8])
        total = part[0] + back[0] + back[1] + back[2]
        dx = (mid.astype(F32) + total).astype(BF)
        return (dx, grads[3], grads[4], grads[5], grads[0], grads[1], grads[2])

    return jax.shard_map(local_step, mesh=mesh, in_specs=(tok_spec,) * 9 + (weight_spec,) * 6, out_specs=(tok_spec,) + (grad_spec,) * 6, check_vma=False)
```

```python
import functools

import jax
import jax.numpy as jnp
from jax import lax
from jax.experimental import pallas as pl
from jax.experimental.pallas import tpu as pltpu
from jax.sharding import PartitionSpec as P

GROUP = 8
EXP = 4
CAP = 24
TOK = 64
DIM = 1024
FFN = 512
PAIR = 2 * CAP
ROWS = GROUP * CAP
NK = 4
KC = DIM // NK
BF = jnp.bfloat16
F32 = jnp.float32
NT = (((1,), (1,)), ((), ()))
TN = (((0,), (0,)), ((), ()))


def dot(a, b, dims=(((1,), (0,)), ((), ()))):
    return lax.dot_general(a, b, dims, preferred_element_type=F32)


class Copy:
    def __init__(self, copy, log):
        self.copy, self.log, self.arrived, self.left = copy, log, False, False

    def start(self):
        self.copy.start()
        self.log.append(self)

    def wait_recv(self):
        self.copy.wait_recv()
        self.arrived = True

    def wait_send(self):
        self.copy.wait_send()
        self.left = True

    def drain(self):
        if not self.arrived:
            self.copy.wait_recv()
        if not self.left:
            self.copy.wait_send()


def exchange_kernel(
    y_hbm, dy_hbm, x_hbm, e2, g2, s2, e1, g1, s1, wg2, wu2, wd2, wg1, wu1, wd1,
    u2, z2, hid2, dab2, u1, z1, hid1, dab1, t1a, t1b, t1c, t1d, dym,
    wcat, wd, tok, dmid, raw_int, raw_gate, route, sel, selt, gate, act, dh, dx, s_oth, s_rcv, s_own, rs_rcv,
    w_sem, l_sem, r_send, r_recv, g_send, g_recv, d_send, d_recv, c_send, c_recv, p_send, p_recv,
):
    me = lax.axis_index("expert")
    core = lax.rem(me, 2)
    bx = lax.rem(me // 2, 2)
    by = me // 4
    partner = me + 1 - 2 * core
    devs = (None, me + 2 - 4 * bx, me + 4 - 8 * by, me + 6 - 4 * bx - 8 * by)
    u, z, hid, dab, t1 = (u1, u2), (z1, z2), (hid1, hid2), (dab1, dab2), (t1a, t1b, t1c, t1d)
    sent = []

    def remote(src, dst, ss, rs, dev):
        copy = pltpu.make_async_remote_copy(
            src_ref=src, dst_ref=dst, send_sem=ss, recv_sem=rs, device_id={"expert": dev}, device_id_type=pl.DeviceIdType.MESH
        )
        return Copy(copy, sent)

    local = [pltpu.make_async_copy(src, tok.at[a, 0], l_sem.at[a]) for a, src in enumerate((y_hbm, dy_hbm, x_hbm))]
    tables = ((e1, raw_int.at[0]), (s1, raw_int.at[1]), (g1, raw_gate.at[0]), (e2, raw_int.at[2]), (s2, raw_int.at[3]), (g2, raw_gate.at[1]))
    tables = [pltpu.make_async_copy(src, dst, l_sem.at[3 + n]) for n, (src, dst) in enumerate(tables)]
    for c in tables + local:
        c.start()
    left, right = pl.ds(0, FFN), pl.ds(FFN, FFN)
    weights = []
    for n, (src, dst) in enumerate(
        (
            (wg2, wcat.at[1, :, :, left]), (wu2, wcat.at[1, :, :, right]), (wd2, wd.at[1]),
            (wg1, wcat.at[0, :, :, left]), (wu1, wcat.at[0, :, :, right]), (wd1, wd.at[0]),
        )
    ):
        weights.append(pltpu.make_async_copy(src, dst, w_sem.at[n]))
    for c in weights[:3]:
        c.start()

    barrier = pltpu.get_barrier_semaphore()
    for dev in (partner,) + devs[1:]:
        pl.semaphore_signal(barrier, inc=1, device_id={"expert": dev}, device_id_type=pl.DeviceIdType.MESH)

    def doubled(v):
        return jnp.concatenate([v, v], axis=1)

    for c in tables:
        c.wait()
    for lay in range(2):
        experts, slots = raw_int[2 * lay], raw_int[2 * lay + 1]
        code = jnp.where(slots >= 0, experts * PAIR + slots, -1000000).astype(F32)
        route[0, 2 * lay] = doubled(code)
        route[0, 2 * lay + 1] = doubled(raw_gate[lay])

    pl.semaphore_wait(barrier, 4)

    class Gather:
        def __init__(self, view, send, recv, relayed=True):
            def move(src, dst, s, r, dev):
                return remote(src, dst, send.at[s], recv.at[r], dev)

            half = (pl.ds(0, TOK // 2), pl.ds(TOK // 2, TOK // 2))
            self.relayed = relayed
            self.own = move(view(0), view(1), 0, 1, partner)
            self.direct = [move(view(0), view(2 * p), p, 2 * p, devs[p]) for p in (1, 2)]
            if relayed:
                self.cross = [
                    move(view(2).at[half[0]], view(6).at[half[0]], 3, 6, devs[2]),
                    move(view(4).at[half[1]], view(6).at[half[1]], 4, 0, devs[1]),
                ]
            else:
                self.cross = [move(view(0), view(6), 3, 6, devs[3])]
            self.passed = [move(view(2 * p), view(2 * p + 1), 4 + p, 2 * p + 1, partner) for p in (1, 2, 3)]

        def launch(self):
            for c in self.direct if self.relayed else self.cross + self.direct:
                c.start()
            self.own.start()

        def relay(self):
            for p in range(2):
                self.direct[p].wait_recv()
                if self.relayed:
                    self.cross[p].start()
                self.passed[p].start()

        def last(self):
            for c in self.cross:
                c.wait_recv()
            self.passed[2].start()

        def rest(self):
            self.own.wait_recv()
            for c in self.passed:
                c.wait_recv()

    routing = Gather(lambda k: route.at[k], r_send, r_recv, relayed=False)
    tokens = [Gather(lambda k, a=a: tok.at[a, k], g_send.at[a], g_recv.at[a]) for a in range(3)]
    routing.launch()
    for a in range(2):
        local[a].wait()
        tokens[a].launch()
    local[2].wait()
    routing.relay()
    routing.last()
    routing.rest()

    lane = lax.broadcasted_iota(jnp.int32, (8, 2 * TOK), 1)
    row = lax.broadcasted_iota(jnp.int32, (EXP * PAIR, 2 * TOK), 0).astype(F32)
    base = (me * (EXP * PAIR)).astype(F32)

    def build_select(lay):
        for p in range(4):
            code = jnp.where(lane < TOK, route[2 * p, 2 * lay], route[2 * p + 1, 2 * lay] + CAP) - base
            gates = jnp.where(lane < TOK, route[2 * p, 2 * lay + 1], route[2 * p + 1, 2 * lay + 1])
            hit = jnp.zeros((EXP * PAIR, 2 * TOK), F32)
            total = jnp.zeros((EXP * PAIR, 2 * TOK), F32)
            for j in range(8):
                match = row == code[j : j + 1, :]
                hit = jnp.where(match, 1.0, hit)
                total = jnp.where(match, gates[j : j + 1, :], total)
            sel[lay, p] = hit.astype(BF)
            selt[lay, p] = hit.T.astype(BF)
            gate[lay, p] = jnp.broadcast_to(jnp.sum(total, axis=1, keepdims=True), (EXP * PAIR, 128))

    build_select(1)
    tokens[0].relay()
    build_select(0)
    tokens[1].relay()
    tokens[2].launch()

    def put_rows(dst, p, cols, rows):
        for e in range(EXP):
            dst[e, p * PAIR : (p + 1) * PAIR, cols] = rows[e * PAIR : (e + 1) * PAIR, :]

    def columns(k):
        return slice(k * KC, (k + 1) * KC)

    def build_u(lay, a, p):
        for k in range(NK):
            block = jnp.concatenate([tok[a, 2 * p, :, columns(k)], tok[a, 2 * p + 1, :, columns(k)]], axis=0)
            put_rows(u[lay], p, columns(k), dot(sel[lay, p], block).astype(BF))

    def build_z(lay, p, k, first, second):
        rows = dot(sel[lay, p], jnp.concatenate([first, second], axis=0))
        g = gate[lay, p]
        rows = jnp.concatenate([rows[:, i * 128 : (i + 1) * 128] * g for i in range(KC // 128)], axis=1)
        put_rows(z[lay], p, columns(k), rows.astype(BF))

    def recompute(lay):
        for e in range(EXP):
            act[e] = dot(u[lay][e], wcat[lay, e]).astype(BF)

    def expert_rows(lay, e, d_hid):
        a = act[e, :, :FFN].astype(F32)
        b = act[e, :, FFN:].astype(F32)
        sig = jax.nn.sigmoid(a)
        silu = a * sig
        hid[lay][e] = (silu * b).astype(BF)
        dab[lay][e, :, :FFN] = (d_hid * b * sig * (1.0 + a * (1.0 - sig))).astype(BF)
        dab[lay][e, :, FFN:] = (d_hid * silu).astype(BF)

    def chip_partial(lay, k):
        for e in range(EXP):
            rows = dot(dab[lay][e], wcat[lay, e, columns(k), :], NT).astype(BF)
            for p in range(4):
                dx[p, e, :, columns(k)] = rows[p * PAIR : (p + 1) * PAIR, :]
        for p in range(4):
            part = dot(selt[lay, p], dx[p, :, :, columns(k)].reshape(EXP * PAIR, KC))
            s_own[lay, k, p] = part[:TOK, :]
            s_oth[lay, k, p] = part[TOK:, :]

    chip = [
        [remote(s_oth.at[lay, k], s_rcv.at[lay, k], c_send.at[lay, k], c_recv.at[lay, k], partner) for k in range(NK)]
        for lay in range(2)
    ]
    scatter = [
        [remote(s_own.at[1, k, p], rs_rcv.at[k, p], p_send.at[k, p], p_recv.at[k, p], devs[p]) for p in (3, 1, 2)]
        for k in range(NK)
    ]

    tokens[0].last()
    tokens[0].rest()
    for p in range(4):
        build_u(1, 0, p)
    weights[0].wait()
    weights[1].wait()
    recompute(1)
    tokens[1].last()
    tokens[1].rest()
    for p in range(4):
        for k in range(NK):
            build_z(1, p, k, tok[1, 2 * p, :, columns(k)], tok[1, 2 * p + 1, :, columns(k)])
    tokens[2].relay()
    weights[2].wait()
    for c in weights[3:]:
        c.start()
    for e in range(EXP):
        expert_rows(1, e, dot(z[1][e], wd[1, e], NT))
    def send_partial(k):
        chip[1][k].wait_recv()
        for p in (3, 1, 2, 0):
            s_own[1, k, p] = s_own[1, k, p] + s_rcv[1, k, p]
        for c in scatter[k]:
            c.start()

    for k in range(NK):
        chip_partial(1, k)
        chip[1][k].start()
        if k:
            send_partial(k - 1)
    send_partial(NK - 1)

    tokens[2].last()
    tokens[2].rest()
    for p in range(4):
        build_u(0, 2, p)
    weights[3].wait()
    weights[4].wait()
    recompute(0)

    middle = [Gather(lambda s, k=k: dmid.at[k, s], d_send.at[k], d_recv.at[k], k < RELAYED) for k in range(NK)]
    for k in range(NK):
        for c in scatter[k]:
            c.wait_recv()
        total = s_own[1, k, 0] + rs_rcv[k, 1] + rs_rcv[k, 2] + rs_rcv[k, 3]
        new = (tok[1, 0, :, columns(k)].astype(F32) + total).astype(BF)
        dmid[k, 0] = new
        dym[:, columns(k)] = new
        middle[k].launch()
    weights[5].wait()

    def hidden_grad(k):
        middle[k].rest()
        for p in range(4):
            build_z(0, p, k, dmid[k, 2 * p], dmid[k, 2 * p + 1])
        for e in range(EXP):
            part = dot(z[0][e, :, columns(k)], wd[0, e, :, columns(k)], NT)
            dh[e] = part if k == 0 else dh[e] + part

    for k in range(NK):
        middle[k].relay()
        if k:
            middle[k - 1].last()
        if k > 1:
            hidden_grad(k - 2)
    middle[NK - 1].last()
    hidden_grad(NK - 2)
    hidden_grad(NK - 1)
    for e in range(EXP):
        expert_rows(0, e, dh[e])
    def last_partial(k):
        chip[0][k].wait_recv()
        for p in range(4):
            t1[p][:, columns(k)] = s_own[0, k, p] + s_rcv[0, k, p]

    for k in range(NK):
        chip_partial(0, k)
        chip[0][k].start()
        if k:
            last_partial(k - 1)
    last_partial(NK - 1)
    for c in sent:
        c.drain()


def exchange(*args):
    rows = lambda n: pltpu.VMEM((EXP, ROWS, n), BF)
    per_layer = [rows(DIM), rows(DIM), rows(FFN), rows(2 * FFN)]
    hbm_spec = pl.BlockSpec(memory_space=pltpu.HBM)
    vmem_spec = pl.BlockSpec(memory_space=pltpu.VMEM)
    dma = pltpu.SemaphoreType.DMA
    return pl.pallas_call(
        exchange_kernel,
        out_shape=per_layer + per_layer + [pltpu.VMEM((TOK, DIM), F32)] * 4 + [pltpu.VMEM((TOK, DIM), BF)],
        in_specs=[hbm_spec] * 15,
        out_specs=[vmem_spec] * 13,
        scratch_shapes=[
            pltpu.VMEM((2, EXP, DIM, 2 * FFN), BF),
            pltpu.VMEM((2, EXP, FFN, DIM), BF),
            pltpu.VMEM((3, GROUP, TOK, DIM), BF),
            pltpu.VMEM((NK, GROUP, TOK, KC), BF),
            pltpu.VMEM((4, 8, TOK), jnp.int32),
            pltpu.VMEM((2, 8, TOK), F32),
            pltpu.VMEM((GROUP, 4, 8, 2 * TOK), F32),
            pltpu.VMEM((2, 4, EXP * PAIR, 2 * TOK), BF),
            pltpu.VMEM((2, 4, 2 * TOK, EXP * PAIR), BF),
            pltpu.VMEM((2, 4, EXP * PAIR, 128), F32),
            pltpu.VMEM((EXP, ROWS, 2 * FFN), BF),
            pltpu.VMEM((EXP, ROWS, FFN), F32),
            pltpu.VMEM((4, EXP, PAIR, DIM), BF),
            pltpu.VMEM((2, NK, 4, TOK, KC), F32),
            pltpu.VMEM((2, NK, 4, TOK, KC), F32),
            pltpu.VMEM((2, NK, 4, TOK, KC), F32),
            pltpu.VMEM((NK, 4, TOK, KC), F32),
            dma((6,)),
            dma((9,)),
            dma((8,)),
            dma((8,)),
            dma((3, 8)),
            dma((3, 8)),
            dma((NK, 8)),
            dma((NK, 8)),
            dma((2, NK)),
            dma((2, NK)),
            dma((NK, 4)),
            dma((NK, 4)),
        ],
        compiler_params=pltpu.CompilerParams(collective_id=0, has_side_effects=True, vmem_limit_bytes=K1_VMEM * 2**20),
        cost_estimate=pl.CostEstimate(flops=10**10, bytes_accessed=40 * 2**20, transcendentals=0),
    )(*[pltpu.with_memory_space_constraint(a, pltpu.HBM) for a in args])


K1_VMEM = 46
RELAYED = 0
MB = 256
SLOTS = 5


def weight_grad_kernel(u2, z2, h2, ab2, u1, z1, h1, ab1, g2, p2, d2, g1, p1, d1, g_buf, p_buf, d_buf, sem):
    flying = {}
    step = 0
    for u, z, h, ab, g_o, p_o, d_o in ((u2, z2, h2, ab2, g2, p2, d2), (u1, z1, h1, ab1, g1, p1, d1)):
        for e in range(EXP):
            slot = step % SLOTS
            for c in flying.pop(step - SLOTS, []):
                c.wait()
            mine = flying.setdefault(step, [])

            def write(buf, out, m, n):
                part = pl.ds(m * MB, MB)
                c = pltpu.make_async_copy(buf.at[slot, part], out.at[e, part], sem.at[slot, n])
                c.start()
                mine.append(c)

            for m in range(DIM // MB):
                span = slice(m * MB, (m + 1) * MB)
                both = dot(u[e, :, span], ab[e], TN)
                g_buf[slot, span, :] = both[:, :FFN]
                p_buf[slot, span, :] = both[:, FFN:]
                write(g_buf, g_o, m, m)
                write(p_buf, p_o, m, DIM // MB + m)
            for m in range(FFN // MB):
                span = slice(m * MB, (m + 1) * MB)
                d_buf[slot, span, :] = dot(h[e, :, span], z[e], TN)
                write(d_buf, d_o, m, 2 * (DIM // MB) + m)
            step += 1
    for cs in flying.values():
        for c in cs:
            c.wait()


def weight_grads(*rows):
    up = jax.ShapeDtypeStruct((EXP, DIM, FFN), F32)
    shapes = [up, up, jax.ShapeDtypeStruct((EXP, FFN, DIM), F32)] * 2
    return pl.pallas_call(
        weight_grad_kernel,
        in_specs=[pl.BlockSpec(memory_space=pltpu.VMEM)] * 8,
        out_specs=[pl.BlockSpec(memory_space=pl.ANY)] * 6,
        out_shape=shapes,
        scratch_shapes=[
            pltpu.VMEM((SLOTS, DIM, FFN), F32),
            pltpu.VMEM((SLOTS, DIM, FFN), F32),
            pltpu.VMEM((SLOTS, FFN, DIM), F32),
            pltpu.SemaphoreType.DMA((SLOTS, 2 * (DIM // MB) + FFN // MB)),
        ],
        compiler_params=pltpu.CompilerParams(vmem_limit_bytes=K2_VMEM * 2**20),
        cost_estimate=pl.CostEstimate(flops=6 * 10**9, bytes_accessed=62 * 2**20, transcendentals=0),
    )(*[pltpu.with_memory_space_constraint(r, pltpu.VMEM) for r in rows])


K2_VMEM = 36


def solution(mesh):
    tok_spec = P(("data", "expert"), None)
    weight_spec = P("expert", None, None)
    grad_spec = P(("data", "expert"), None, None)

    def local_step(x_tokens, y_mid, dy_out, experts_one, gates_one, slots_one, experts_two, gates_two, slots_two, w_gate_one, w_up_one, w_down_one, w_gate_two, w_up_two, w_down_two):
        res = exchange(
            y_mid, dy_out, x_tokens, experts_two.T, gates_two.T, slots_two.T, experts_one.T, gates_one.T, slots_one.T,
            w_gate_two, w_up_two, w_down_two, w_gate_one, w_up_one, w_down_one,
        )
        part, mid = res[8:12], res[12]
        back = [lax.ppermute(part[p], "expert", [(i, i ^ (2 * p)) for i in range(GROUP)]) for p in (1, 2, 3)]
        grads = weight_grads(*res[:8])
        total = part[0] + back[0] + back[1] + back[2]
        dx = (mid.astype(F32) + total).astype(BF)
        return (dx, grads[3], grads[4], grads[5], grads[0], grads[1], grads[2])

    return jax.shard_map(local_step, mesh=mesh, in_specs=(tok_spec,) * 9 + (weight_spec,) * 6, out_specs=(tok_spec,) + (grad_spec,) * 6, check_vma=False)
```

```python
import functools

import jax
import jax.numpy as jnp
from jax import lax
from jax.experimental import pallas as pl
from jax.experimental.pallas import tpu as pltpu
from jax.sharding import PartitionSpec as P

GROUP = 8
EXP = 4
CAP = 24
TOK = 64
DIM = 1024
FFN = 512
PAIR = 2 * CAP
ROWS = GROUP * CAP
NK = 4
KC = DIM // NK
BF = jnp.bfloat16
F32 = jnp.float32
TN = (((0,), (0,)), ((), ()))


def dot(a, b, dims=(((1,), (0,)), ((), ()))):
    return lax.dot_general(a, b, dims, preferred_element_type=F32)


class Copy:
    def __init__(self, copy, log):
        self.copy, self.log, self.arrived, self.left = copy, log, False, False

    def start(self):
        self.copy.start()
        self.log.append(self)

    def wait_recv(self):
        self.copy.wait_recv()
        self.arrived = True

    def wait_send(self):
        self.copy.wait_send()
        self.left = True

    def drain(self):
        if not self.arrived:
            self.copy.wait_recv()
        if not self.left:
            self.copy.wait_send()


def exchange_kernel(
    y_hbm, dy_hbm, x_hbm, e2, g2, s2, e1, g1, s1, wg2, wu2, wd2, wg1, wu1, wd1,
    u2, z2, hid2, dab2, u1, z1, hid1, dab1, t1a, t1b, t1c, t1d, dym,
    wcat, wd, wcat_t, wd_t, tok, dmid, raw_int, raw_gate, route, sel, selt, gate, act, dh, dx, s_oth, s_rcv, s_own, rs_rcv,
    w_sem, l_sem, r_send, r_recv, g_send, g_recv, d_send, d_recv, c_send, c_recv, p_send, p_recv,
):
    me = lax.axis_index("expert")
    core = lax.rem(me, 2)
    bx = lax.rem(me // 2, 2)
    by = me // 4
    partner = me + 1 - 2 * core
    devs = (None, me + 2 - 4 * bx, me + 4 - 8 * by, me + 6 - 4 * bx - 8 * by)
    u, z, hid, dab, t1 = (u1, u2), (z1, z2), (hid1, hid2), (dab1, dab2), (t1a, t1b, t1c, t1d)
    sent = []

    def remote(src, dst, ss, rs, dev):
        copy = pltpu.make_async_remote_copy(
            src_ref=src, dst_ref=dst, send_sem=ss, recv_sem=rs, device_id={"expert": dev}, device_id_type=pl.DeviceIdType.MESH
        )
        return Copy(copy, sent)

    local = [pltpu.make_async_copy(src, tok.at[a, 0], l_sem.at[a]) for a, src in enumerate((y_hbm, dy_hbm, x_hbm))]
    tables = ((e1, raw_int.at[0]), (s1, raw_int.at[1]), (g1, raw_gate.at[0]), (e2, raw_int.at[2]), (s2, raw_int.at[3]), (g2, raw_gate.at[1]))
    tables = [pltpu.make_async_copy(src, dst, l_sem.at[3 + n]) for n, (src, dst) in enumerate(tables)]
    for c in tables + local:
        c.start()
    left, right = pl.ds(0, FFN), pl.ds(FFN, FFN)
    weights = []
    for n, (src, dst) in enumerate(
        (
            (wg2, wcat.at[:, :, left]), (wu2, wcat.at[:, :, right]), (wd2, wd),
            (wg1, wcat.at[:, :, left]), (wu1, wcat.at[:, :, right]), (wd1, wd),
        )
    ):
        weights.append(pltpu.make_async_copy(src, dst, w_sem.at[n]))
    for c in weights[:3]:
        c.start()

    barrier = pltpu.get_barrier_semaphore()
    for dev in (partner,) + devs[1:]:
        pl.semaphore_signal(barrier, inc=1, device_id={"expert": dev}, device_id_type=pl.DeviceIdType.MESH)

    def doubled(v):
        return jnp.concatenate([v, v], axis=1)

    for c in tables:
        c.wait()
    for lay in range(2):
        experts, slots = raw_int[2 * lay], raw_int[2 * lay + 1]
        code = jnp.where(slots >= 0, experts * PAIR + slots, -1000000).astype(F32)
        route[0, 2 * lay] = doubled(code)
        route[0, 2 * lay + 1] = doubled(raw_gate[lay])

    pl.semaphore_wait(barrier, 4)

    class Gather:
        def __init__(self, view, send, recv, relayed=True):
            def move(src, dst, s, r, dev):
                return remote(src, dst, send.at[s], recv.at[r], dev)

            half = (pl.ds(0, TOK // 2), pl.ds(TOK // 2, TOK // 2))
            self.relayed = relayed
            self.own = move(view(0), view(1), 0, 1, partner)
            self.direct = [move(view(0), view(2 * p), p, 2 * p, devs[p]) for p in (1, 2)]
            if relayed:
                self.cross = [
                    move(view(2).at[half[0]], view(6).at[half[0]], 3, 6, devs[2]),
                    move(view(4).at[half[1]], view(6).at[half[1]], 4, 0, devs[1]),
                ]
            else:
                self.cross = [move(view(0), view(6), 3, 6, devs[3])]
            self.passed = [move(view(2 * p), view(2 * p + 1), 4 + p, 2 * p + 1, partner) for p in (1, 2, 3)]

        def launch(self):
            for c in self.direct if self.relayed else self.cross + self.direct:
                c.start()
            self.own.start()

        def relay(self):
            for p in range(2):
                self.direct[p].wait_recv()
                if self.relayed:
                    self.cross[p].start()
                self.passed[p].start()

        def last(self):
            for c in self.cross:
                c.wait_recv()
            self.passed[2].start()

        def rest(self):
            self.own.wait_recv()
            for c in self.passed:
                c.wait_recv()

    def transpose_weights():
        for e in range(EXP):
            for i in range(DIM // TR):
                for j in range(2 * FFN // TR):
                    wcat_t[e, j * TR : (j + 1) * TR, i * TR : (i + 1) * TR] = wcat[e, i * TR : (i + 1) * TR, j * TR : (j + 1) * TR].T
                for j in range(FFN // TR):
                    wd_t[e, i * TR : (i + 1) * TR, j * TR : (j + 1) * TR] = wd[e, j * TR : (j + 1) * TR, i * TR : (i + 1) * TR].T

    routing = Gather(lambda k: route.at[k], r_send, r_recv, relayed=False)
    tokens = [Gather(lambda k, a=a: tok.at[a, k], g_send.at[a], g_recv.at[a]) for a in range(3)]
    routing.launch()
    for a in range(2):
        local[a].wait()
        tokens[a].launch()
    local[2].wait()
    for c in weights[:3]:
        c.wait()
    transpose_weights()
    routing.relay()
    routing.last()
    routing.rest()

    lane = lax.broadcasted_iota(jnp.int32, (8, 2 * TOK), 1)
    row = lax.broadcasted_iota(jnp.int32, (EXP * PAIR, 2 * TOK), 0).astype(F32)
    base = (me * (EXP * PAIR)).astype(F32)

    def build_select(lay):
        for p in range(4):
            code = jnp.where(lane < TOK, route[2 * p, 2 * lay], route[2 * p + 1, 2 * lay] + CAP) - base
            gates = jnp.where(lane < TOK, route[2 * p, 2 * lay + 1], route[2 * p + 1, 2 * lay + 1])
            hit = jnp.zeros((EXP * PAIR, 2 * TOK), F32)
            total = jnp.zeros((EXP * PAIR, 2 * TOK), F32)
            for j in range(8):
                match = row == code[j : j + 1, :]
                hit = jnp.where(match, 1.0, hit)
                total = jnp.where(match, gates[j : j + 1, :], total)
            sel[lay, p] = hit.astype(BF)
            selt[lay, p] = hit.T.astype(BF)
            gate[lay, p] = jnp.broadcast_to(jnp.sum(total, axis=1, keepdims=True), (EXP * PAIR, 128))

    build_select(1)
    tokens[0].relay()
    build_select(0)
    tokens[1].relay()
    tokens[2].launch()

    def put_rows(dst, p, cols, rows):
        for e in range(EXP):
            dst[e, p * PAIR : (p + 1) * PAIR, cols] = rows[e * PAIR : (e + 1) * PAIR, :]

    def columns(k):
        return slice(k * KC, (k + 1) * KC)

    def build_u(lay, a, p):
        for k in range(NK):
            block = jnp.concatenate([tok[a, 2 * p, :, columns(k)], tok[a, 2 * p + 1, :, columns(k)]], axis=0)
            put_rows(u[lay], p, columns(k), dot(sel[lay, p], block).astype(BF))

    def build_z(lay, p, k, first, second):
        rows = dot(sel[lay, p], jnp.concatenate([first, second], axis=0))
        g = gate[lay, p]
        rows = jnp.concatenate([rows[:, i * 128 : (i + 1) * 128] * g for i in range(KC // 128)], axis=1)
        put_rows(z[lay], p, columns(k), rows.astype(BF))

    def recompute(lay):
        for e in range(EXP):
            act[e] = dot(u[lay][e], wcat[e]).astype(BF)

    def expert_rows(lay, e, d_hid):
        a = act[e, :, :FFN].astype(F32)
        b = act[e, :, FFN:].astype(F32)
        sig = jax.nn.sigmoid(a)
        silu = a * sig
        hid[lay][e] = (silu * b).astype(BF)
        dab[lay][e, :, :FFN] = (d_hid * b * sig * (1.0 + a * (1.0 - sig))).astype(BF)
        dab[lay][e, :, FFN:] = (d_hid * silu).astype(BF)

    def chip_partial(lay, k):
        for e in range(EXP):
            rows = dot(dab[lay][e], wcat_t[e, :, columns(k)]).astype(BF)
            for p in range(4):
                dx[p, e, :, columns(k)] = rows[p * PAIR : (p + 1) * PAIR, :]
        for p in range(4):
            part = dot(selt[lay, p], dx[p, :, :, columns(k)].reshape(EXP * PAIR, KC))
            s_own[lay, k, p] = part[:TOK, :]
            s_oth[lay, k, p] = part[TOK:, :]

    chip = [
        [remote(s_oth.at[lay, k], s_rcv.at[lay, k], c_send.at[lay, k], c_recv.at[lay, k], partner) for k in range(NK)]
        for lay in range(2)
    ]
    first = [1 + k % 2 for k in range(NK)]

    def toward(k, p, slot, dev):
        return remote(s_own.at[1, k, p], rs_rcv.at[k, slot], p_send.at[k, slot], p_recv.at[k, slot], devs[dev])

    scatter = [[toward(k, 3, 1, first[k]), toward(k, first[k], 0, first[k])] for k in range(NK)]
    onward = [toward(k, 3 - first[k], 2, 3 - first[k]) for k in range(NK)]

    def relay_partial(k):
        scatter[k][0].wait_recv()
        p = 3 - first[k]
        s_own[1, k, p] = s_own[1, k, p] + rs_rcv[k, 1]
        onward[k].start()

    tokens[0].last()
    tokens[0].rest()
    for p in range(4):
        build_u(1, 0, p)
    recompute(1)
    for c in weights[3:]:
        c.start()
    tokens[1].last()
    tokens[1].rest()
    for p in range(4):
        for k in range(NK):
            build_z(1, p, k, tok[1, 2 * p, :, columns(k)], tok[1, 2 * p + 1, :, columns(k)])
    tokens[2].relay()
    for e in range(EXP):
        expert_rows(1, e, dot(z[1][e], wd_t[e]))
    def send_partial(k):
        chip[1][k].wait_recv()
        for p in (3, 1, 2, 0):
            s_own[1, k, p] = s_own[1, k, p] + s_rcv[1, k, p]
        for c in scatter[k]:
            c.start()

    for k in range(NK):
        chip_partial(1, k)
        chip[1][k].start()
        if k:
            send_partial(k - 1)
    send_partial(NK - 1)

    relay_partial(0)
    relay_partial(1)
    tokens[2].last()
    tokens[2].rest()
    for p in range(4):
        build_u(0, 2, p)
    for c in weights[3:]:
        c.wait()
    relay_partial(2)
    relay_partial(3)
    recompute(0)

    middle = [Gather(lambda s, k=k: dmid.at[k, s], d_send.at[k], d_recv.at[k], k < RELAYED) for k in range(NK)]
    for k in range(NK):
        scatter[k][1].wait_recv()
        onward[k].wait_recv()
        total = s_own[1, k, 0] + rs_rcv[k, 0] + rs_rcv[k, 2]
        new = (tok[1, 0, :, columns(k)].astype(F32) + total).astype(BF)
        dmid[k, 0] = new
        dym[:, columns(k)] = new
        middle[k].launch()
    transpose_weights()

    def hidden_grad(k):
        middle[k].rest()
        for p in range(4):
            build_z(0, p, k, dmid[k, 2 * p], dmid[k, 2 * p + 1])
        for e in range(EXP):
            part = dot(z[0][e, :, columns(k)], wd_t[e, columns(k), :])
            dh[e] = part if k == 0 else dh[e] + part

    for k in range(NK):
        middle[k].relay()
        if k:
            middle[k - 1].last()
        if k > 1:
            hidden_grad(k - 2)
    middle[NK - 1].last()
    hidden_grad(NK - 2)
    hidden_grad(NK - 1)
    for e in range(EXP):
        expert_rows(0, e, dh[e])
    def last_partial(k):
        chip[0][k].wait_recv()
        for p in range(4):
            t1[p][:, columns(k)] = s_own[0, k, p] + s_rcv[0, k, p]

    for k in range(NK):
        chip_partial(0, k)
        chip[0][k].start()
        if k:
            last_partial(k - 1)
    last_partial(NK - 1)
    for c in sent:
        c.drain()


def exchange(*args):
    rows = lambda n: pltpu.VMEM((EXP, ROWS, n), BF)
    per_layer = [rows(DIM), rows(DIM), rows(FFN), rows(2 * FFN)]
    hbm_spec = pl.BlockSpec(memory_space=pltpu.HBM)
    vmem_spec = pl.BlockSpec(memory_space=pltpu.VMEM)
    dma = pltpu.SemaphoreType.DMA
    return pl.pallas_call(
        exchange_kernel,
        out_shape=per_layer + per_layer + [pltpu.VMEM((TOK, DIM), F32)] * 4 + [pltpu.VMEM((TOK, DIM), BF)],
        in_specs=[hbm_spec] * 15,
        out_specs=[vmem_spec] * 13,
        scratch_shapes=[
            pltpu.VMEM((EXP, DIM, 2 * FFN), BF),
            pltpu.VMEM((EXP, FFN, DIM), BF),
            pltpu.VMEM((EXP, 2 * FFN, DIM), BF),
            pltpu.VMEM((EXP, DIM, FFN), BF),
            pltpu.VMEM((3, GROUP, TOK, DIM), BF),
            pltpu.VMEM((NK, GROUP, TOK, KC), BF),
            pltpu.VMEM((4, 8, TOK), jnp.int32),
            pltpu.VMEM((2, 8, TOK), F32),
            pltpu.VMEM((GROUP, 4, 8, 2 * TOK), F32),
            pltpu.VMEM((2, 4, EXP * PAIR, 2 * TOK), BF),
            pltpu.VMEM((2, 4, 2 * TOK, EXP * PAIR), BF),
            pltpu.VMEM((2, 4, EXP * PAIR, 128), F32),
            pltpu.VMEM((EXP, ROWS, 2 * FFN), BF),
            pltpu.VMEM((EXP, ROWS, FFN), F32),
            pltpu.VMEM((4, EXP, PAIR, DIM), BF),
            pltpu.VMEM((2, NK, 4, TOK, KC), F32),
            pltpu.VMEM((2, NK, 4, TOK, KC), F32),
            pltpu.VMEM((2, NK, 4, TOK, KC), F32),
            pltpu.VMEM((NK, 4, TOK, KC), F32),
            dma((6,)),
            dma((9,)),
            dma((8,)),
            dma((8,)),
            dma((3, 8)),
            dma((3, 8)),
            dma((NK, 8)),
            dma((NK, 8)),
            dma((2, NK)),
            dma((2, NK)),
            dma((NK, 4)),
            dma((NK, 4)),
        ],
        compiler_params=pltpu.CompilerParams(collective_id=0, has_side_effects=True, vmem_limit_bytes=K1_VMEM * 2**20),
        cost_estimate=pl.CostEstimate(flops=10**10, bytes_accessed=40 * 2**20, transcendentals=0),
    )(*[pltpu.with_memory_space_constraint(a, pltpu.HBM) for a in args])


K1_VMEM = 46
RELAYED = 0
TR = 256
MB = 256
SLOTS = 5


def weight_grad_kernel(u2, z2, h2, ab2, u1, z1, h1, ab1, g2, p2, d2, g1, p1, d1, g_buf, p_buf, d_buf, sem):
    flying = {}
    step = 0
    for u, z, h, ab, g_o, p_o, d_o in ((u2, z2, h2, ab2, g2, p2, d2), (u1, z1, h1, ab1, g1, p1, d1)):
        for e in range(EXP):
            slot = step % SLOTS
            for c in flying.pop(step - SLOTS, []):
                c.wait()
            mine = flying.setdefault(step, [])

            def write(buf, out, m, n):
                part = pl.ds(m * MB, MB)
                c = pltpu.make_async_copy(buf.at[slot, part], out.at[e, part], sem.at[slot, n])
                c.start()
                mine.append(c)

            for m in range(DIM // MB):
                span = slice(m * MB, (m + 1) * MB)
                both = dot(u[e, :, span], ab[e], TN)
                g_buf[slot, span, :] = both[:, :FFN]
                p_buf[slot, span, :] = both[:, FFN:]
                write(g_buf, g_o, m, m)
                write(p_buf, p_o, m, DIM // MB + m)
            for m in range(FFN // MB):
                span = slice(m * MB, (m + 1) * MB)
                d_buf[slot, span, :] = dot(h[e, :, span], z[e], TN)
                write(d_buf, d_o, m, 2 * (DIM // MB) + m)
            step += 1
    for cs in flying.values():
        for c in cs:
            c.wait()


def weight_grads(*rows):
    up = jax.ShapeDtypeStruct((EXP, DIM, FFN), F32)
    shapes = [up, up, jax.ShapeDtypeStruct((EXP, FFN, DIM), F32)] * 2
    return pl.pallas_call(
        weight_grad_kernel,
        in_specs=[pl.BlockSpec(memory_space=pltpu.VMEM)] * 8,
        out_specs=[pl.BlockSpec(memory_space=pl.ANY)] * 6,
        out_shape=shapes,
        scratch_shapes=[
            pltpu.VMEM((SLOTS, DIM, FFN), F32),
            pltpu.VMEM((SLOTS, DIM, FFN), F32),
            pltpu.VMEM((SLOTS, FFN, DIM), F32),
            pltpu.SemaphoreType.DMA((SLOTS, 2 * (DIM // MB) + FFN // MB)),
        ],
        compiler_params=pltpu.CompilerParams(vmem_limit_bytes=K2_VMEM * 2**20),
        cost_estimate=pl.CostEstimate(flops=6 * 10**9, bytes_accessed=62 * 2**20, transcendentals=0),
    )(*[pltpu.with_memory_space_constraint(r, pltpu.VMEM) for r in rows])


K2_VMEM = 36


def solution(mesh):
    tok_spec = P(("data", "expert"), None)
    weight_spec = P("expert", None, None)
    grad_spec = P(("data", "expert"), None, None)

    def local_step(x_tokens, y_mid, dy_out, experts_one, gates_one, slots_one, experts_two, gates_two, slots_two, w_gate_one, w_up_one, w_down_one, w_gate_two, w_up_two, w_down_two):
        res = exchange(
            y_mid, dy_out, x_tokens, experts_two.T, gates_two.T, slots_two.T, experts_one.T, gates_one.T, slots_one.T,
            w_gate_two, w_up_two, w_down_two, w_gate_one, w_up_one, w_down_one,
        )
        part, mid = res[8:12], res[12]
        back = [lax.ppermute(part[p], "expert", [(i, i ^ (2 * p)) for i in range(GROUP)]) for p in (1, 2, 3)]
        grads = weight_grads(*res[:8])
        total = part[0] + back[0] + back[1] + back[2]
        dx = (mid.astype(F32) + total).astype(BF)
        return (dx, grads[3], grads[4], grads[5], grads[0], grads[1], grads[2])

    return jax.shard_map(local_step, mesh=mesh, in_specs=(tok_spec,) * 9 + (weight_spec,) * 6, out_specs=(tok_spec,) + (grad_spec,) * 6, check_vma=False)
```

```python
import functools

import jax
import jax.numpy as jnp
from jax import lax
from jax.experimental import pallas as pl
from jax.experimental.pallas import tpu as pltpu
from jax.sharding import PartitionSpec as P

GROUP = 8
EXP = 4
CAP = 24
TOK = 64
DIM = 1024
FFN = 512
PAIR = 2 * CAP
ROWS = GROUP * CAP
NK = 4
KC = DIM // NK
BF = jnp.bfloat16
F32 = jnp.float32
TN = (((0,), (0,)), ((), ()))


def dot(a, b, dims=(((1,), (0,)), ((), ()))):
    return lax.dot_general(a, b, dims, preferred_element_type=F32)


class Copy:
    def __init__(self, copy, log):
        self.copy, self.log, self.arrived, self.left = copy, log, False, False

    def start(self):
        self.copy.start()
        self.log.append(self)

    def wait_recv(self):
        self.copy.wait_recv()
        self.arrived = True

    def wait_send(self):
        self.copy.wait_send()
        self.left = True

    def drain(self):
        if not self.arrived:
            self.copy.wait_recv()
        if not self.left:
            self.copy.wait_send()


def exchange_kernel(
    y_hbm, dy_hbm, x_hbm, e2, g2, s2, e1, g1, s1, wg2, wu2, wd2, wg1, wu1, wd1,
    u2, z2, hid2, dab2, u1, z1, hid1, dab1, t1a, t1b, t1c, t1d, dym,
    wcat, wd, wcat_t, wd_t, tok, dmid, raw_int, raw_gate, route, sel, selt, gate, act, dh, dx, s_oth, s_rcv, s_own, rs_rcv,
    w_sem, l_sem, r_send, r_recv, g_send, g_recv, d_send, d_recv, c_send, c_recv, p_send, p_recv,
):
    me = lax.axis_index("expert")
    core = lax.rem(me, 2)
    bx = lax.rem(me // 2, 2)
    by = me // 4
    partner = me + 1 - 2 * core
    devs = (None, me + 2 - 4 * bx, me + 4 - 8 * by, me + 6 - 4 * bx - 8 * by)
    u, z, hid, dab, t1 = (u1, u2), (z1, z2), (hid1, hid2), (dab1, dab2), (t1a, t1b, t1c, t1d)
    sent = []

    def remote(src, dst, ss, rs, dev):
        copy = pltpu.make_async_remote_copy(
            src_ref=src, dst_ref=dst, send_sem=ss, recv_sem=rs, device_id={"expert": dev}, device_id_type=pl.DeviceIdType.MESH
        )
        return Copy(copy, sent)

    local = [pltpu.make_async_copy(src, tok.at[a, 0], l_sem.at[a]) for a, src in enumerate((y_hbm, dy_hbm, x_hbm))]
    tables = ((e1, raw_int.at[0]), (s1, raw_int.at[1]), (g1, raw_gate.at[0]), (e2, raw_int.at[2]), (s2, raw_int.at[3]), (g2, raw_gate.at[1]))
    tables = [pltpu.make_async_copy(src, dst, l_sem.at[3 + n]) for n, (src, dst) in enumerate(tables)]
    for c in tables + local:
        c.start()
    left, right = pl.ds(0, FFN), pl.ds(FFN, FFN)
    weights = []
    for n, (src, dst) in enumerate(
        (
            (wg2, wcat.at[:, :, left]), (wu2, wcat.at[:, :, right]), (wd2, wd),
            (wg1, wcat.at[:, :, left]), (wu1, wcat.at[:, :, right]), (wd1, wd),
        )
    ):
        weights.append(pltpu.make_async_copy(src, dst, w_sem.at[n]))
    for c in weights[:3]:
        c.start()

    barrier = pltpu.get_barrier_semaphore()
    for dev in (partner,) + devs[1:]:
        pl.semaphore_signal(barrier, inc=1, device_id={"expert": dev}, device_id_type=pl.DeviceIdType.MESH)

    def doubled(v):
        return jnp.concatenate([v, v], axis=1)

    for c in tables:
        c.wait()
    for lay in range(2):
        experts, slots = raw_int[2 * lay], raw_int[2 * lay + 1]
        code = jnp.where(slots >= 0, experts * PAIR + slots, -1000000).astype(F32)
        route[0, 2 * lay] = doubled(code)
        route[0, 2 * lay + 1] = doubled(raw_gate[lay])

    pl.semaphore_wait(barrier, 4)

    class Gather:
        def __init__(self, view, send, recv, relayed=True):
            def move(src, dst, s, r, dev):
                return remote(src, dst, send.at[s], recv.at[r], dev)

            half = (pl.ds(0, TOK // 2), pl.ds(TOK // 2, TOK // 2))
            self.relayed = relayed
            self.own = move(view(0), view(1), 0, 1, partner)
            self.direct = [move(view(0), view(2 * p), p, 2 * p, devs[p]) for p in (1, 2)]
            if relayed:
                self.cross = [
                    move(view(2).at[half[0]], view(6).at[half[0]], 3, 6, devs[2]),
                    move(view(4).at[half[1]], view(6).at[half[1]], 4, 0, devs[1]),
                ]
            else:
                self.cross = [move(view(0), view(6), 3, 6, devs[3])]
            self.passed = [move(view(2 * p), view(2 * p + 1), 4 + p, 2 * p + 1, partner) for p in (1, 2, 3)]

        def launch(self):
            for c in self.direct if self.relayed else self.cross + self.direct:
                c.start()
            self.own.start()

        def relay(self):
            for p in range(2):
                self.direct[p].wait_recv()
                if self.relayed:
                    self.cross[p].start()
                self.passed[p].start()

        def last(self):
            for c in self.cross:
                c.wait_recv()
            self.passed[2].start()

        def rest(self):
            self.own.wait_recv()
            for c in self.passed:
                c.wait_recv()

    def transpose_weights():
        for e in range(EXP):
            for i in range(DIM // TR):
                for j in range(2 * FFN // TR):
                    wcat_t[e, j * TR : (j + 1) * TR, i * TR : (i + 1) * TR] = wcat[e, i * TR : (i + 1) * TR, j * TR : (j + 1) * TR].T
                for j in range(FFN // TR):
                    wd_t[e, i * TR : (i + 1) * TR, j * TR : (j + 1) * TR] = wd[e, j * TR : (j + 1) * TR, i * TR : (i + 1) * TR].T

    routing = Gather(lambda k: route.at[k], r_send, r_recv, relayed=False)
    tokens = [Gather(lambda k, a=a: tok.at[a, k], g_send.at[a], g_recv.at[a]) for a in range(3)]
    routing.launch()
    for a in range(2):
        local[a].wait()
        tokens[a].launch()
    local[2].wait()
    for c in weights[:3]:
        c.wait()
    transpose_weights()
    routing.relay()
    routing.last()
    routing.rest()

    lane = lax.broadcasted_iota(jnp.int32, (8, 2 * TOK), 1)
    row = lax.broadcasted_iota(jnp.int32, (EXP * PAIR, 2 * TOK), 0).astype(F32)
    base = (me * (EXP * PAIR)).astype(F32)

    def build_select(lay):
        for p in range(4):
            code = jnp.where(lane < TOK, route[2 * p, 2 * lay], route[2 * p + 1, 2 * lay] + CAP) - base
            gates = jnp.where(lane < TOK, route[2 * p, 2 * lay + 1], route[2 * p + 1, 2 * lay + 1])
            hit = jnp.zeros((EXP * PAIR, 2 * TOK), F32)
            total = jnp.zeros((EXP * PAIR, 2 * TOK), F32)
            for j in range(8):
                match = row == code[j : j + 1, :]
                hit = jnp.where(match, 1.0, hit)
                total = jnp.where(match, gates[j : j + 1, :], total)
            sel[lay, p] = hit.astype(BF)
            selt[lay, p] = hit.T.astype(BF)
            gate[lay, p] = jnp.broadcast_to(jnp.sum(total, axis=1, keepdims=True), (EXP * PAIR, 128))

    build_select(1)
    tokens[0].relay()
    build_select(0)
    tokens[1].relay()
    tokens[2].launch()
    tokens[0].last()

    def put_rows(dst, p, cols, rows):
        for e in range(EXP):
            dst[e, p * PAIR : (p + 1) * PAIR, cols] = rows[e * PAIR : (e + 1) * PAIR, :]

    def columns(k):
        return slice(k * KC, (k + 1) * KC)

    def build_u(lay, a, p):
        for k in range(NK):
            block = jnp.concatenate([tok[a, 2 * p, :, columns(k)], tok[a, 2 * p + 1, :, columns(k)]], axis=0)
            put_rows(u[lay], p, columns(k), dot(sel[lay, p], block).astype(BF))

    def build_z(lay, p, k, first, second):
        rows = dot(sel[lay, p], jnp.concatenate([first, second], axis=0))
        g = gate[lay, p]
        rows = jnp.concatenate([rows[:, i * 128 : (i + 1) * 128] * g for i in range(KC // 128)], axis=1)
        put_rows(z[lay], p, columns(k), rows.astype(BF))

    def recompute(lay):
        for e in range(EXP):
            act[e] = dot(u[lay][e], wcat[e]).astype(BF)

    def expert_rows(lay, e, d_hid):
        a = act[e, :, :FFN].astype(F32)
        b = act[e, :, FFN:].astype(F32)
        sig = jax.nn.sigmoid(a)
        silu = a * sig
        hid[lay][e] = (silu * b).astype(BF)
        dab[lay][e, :, :FFN] = (d_hid * b * sig * (1.0 + a * (1.0 - sig))).astype(BF)
        dab[lay][e, :, FFN:] = (d_hid * silu).astype(BF)

    def chip_partial(lay, k):
        for e in range(EXP):
            rows = dot(dab[lay][e], wcat_t[e, :, columns(k)]).astype(BF)
            for p in range(4):
                dx[p, e, :, columns(k)] = rows[p * PAIR : (p + 1) * PAIR, :]
        for p in range(4):
            part = dot(selt[lay, p], dx[p, :, :, columns(k)].reshape(EXP * PAIR, KC))
            s_own[lay, k, p] = part[:TOK, :]
            s_oth[lay, k, p] = part[TOK:, :]

    chip = [
        [remote(s_oth.at[lay, k], s_rcv.at[lay, k], c_send.at[lay, k], c_recv.at[lay, k], partner) for k in range(NK)]
        for lay in range(2)
    ]
    first = [1 + k % 2 for k in range(NK)]

    def toward(k, p, slot, dev):
        return remote(s_own.at[1, k, p], rs_rcv.at[k, slot], p_send.at[k, slot], p_recv.at[k, slot], devs[dev])

    scatter = [[toward(k, 3, 1, first[k]), toward(k, first[k], 0, first[k])] for k in range(NK)]
    onward = [toward(k, 3 - first[k], 2, 3 - first[k]) for k in range(NK)]

    def relay_partial(k):
        scatter[k][0].wait_recv()
        p = 3 - first[k]
        s_own[1, k, p] = s_own[1, k, p] + rs_rcv[k, 1]
        onward[k].start()

    tokens[0].rest()
    for p in range(4):
        build_u(1, 0, p)
    recompute(1)
    for c in weights[3:]:
        c.start()
    tokens[1].last()
    tokens[2].relay()
    tokens[1].rest()
    for p in range(4):
        for k in range(NK):
            build_z(1, p, k, tok[1, 2 * p, :, columns(k)], tok[1, 2 * p + 1, :, columns(k)])
    for e in range(EXP):
        expert_rows(1, e, dot(z[1][e], wd_t[e]))
    def send_partial(k):
        chip[1][k].wait_recv()
        for p in (3, 1, 2, 0):
            s_own[1, k, p] = s_own[1, k, p] + s_rcv[1, k, p]
        for c in scatter[k]:
            c.start()

    for k in range(NK):
        chip_partial(1, k)
        chip[1][k].start()
        if k:
            send_partial(k - 1)
    send_partial(NK - 1)

    relay_partial(0)
    relay_partial(1)
    tokens[2].last()
    tokens[2].rest()
    for p in range(4):
        build_u(0, 2, p)
    for c in weights[3:]:
        c.wait()
    relay_partial(2)
    relay_partial(3)
    recompute(0)

    middle = [Gather(lambda s, k=k: dmid.at[k, s], d_send.at[k], d_recv.at[k], k < RELAYED) for k in range(NK)]
    for k in range(NK):
        scatter[k][1].wait_recv()
        onward[k].wait_recv()
        total = s_own[1, k, 0] + rs_rcv[k, 0] + rs_rcv[k, 2]
        new = (tok[1, 0, :, columns(k)].astype(F32) + total).astype(BF)
        dmid[k, 0] = new
        dym[:, columns(k)] = new
        middle[k].launch()
    transpose_weights()

    def hidden_grad(k):
        middle[k].rest()
        for p in range(4):
            build_z(0, p, k, dmid[k, 2 * p], dmid[k, 2 * p + 1])
        for e in range(EXP):
            part = dot(z[0][e, :, columns(k)], wd_t[e, columns(k), :])
            if k == NK - 1:
                expert_rows(0, e, dh[e] + part)
            else:
                dh[e] = part if k == 0 else dh[e] + part

    for k in range(NK):
        middle[k].relay()
        if k:
            middle[k - 1].last()
        if k > 1:
            hidden_grad(k - 2)
    middle[NK - 1].last()
    hidden_grad(NK - 2)
    hidden_grad(NK - 1)
    def last_partial(k):
        chip[0][k].wait_recv()
        for p in range(4):
            t1[p][:, columns(k)] = s_own[0, k, p] + s_rcv[0, k, p]

    for k in range(NK):
        chip_partial(0, k)
        chip[0][k].start()
        if k:
            last_partial(k - 1)
    last_partial(NK - 1)
    for c in sent:
        c.drain()


def exchange(*args):
    rows = lambda n: pltpu.VMEM((EXP, ROWS, n), BF)
    per_layer = [rows(DIM), rows(DIM), rows(FFN), rows(2 * FFN)]
    hbm_spec = pl.BlockSpec(memory_space=pltpu.HBM)
    vmem_spec = pl.BlockSpec(memory_space=pltpu.VMEM)
    dma = pltpu.SemaphoreType.DMA
    return pl.pallas_call(
        exchange_kernel,
        out_shape=per_layer + per_layer + [pltpu.VMEM((TOK, DIM), F32)] * 4 + [pltpu.VMEM((TOK, DIM), BF)],
        in_specs=[hbm_spec] * 15,
        out_specs=[vmem_spec] * 13,
        scratch_shapes=[
            pltpu.VMEM((EXP, DIM, 2 * FFN), BF),
            pltpu.VMEM((EXP, FFN, DIM), BF),
            pltpu.VMEM((EXP, 2 * FFN, DIM), BF),
            pltpu.VMEM((EXP, DIM, FFN), BF),
            pltpu.VMEM((3, GROUP, TOK, DIM), BF),
            pltpu.VMEM((NK, GROUP, TOK, KC), BF),
            pltpu.VMEM((4, 8, TOK), jnp.int32),
            pltpu.VMEM((2, 8, TOK), F32),
            pltpu.VMEM((GROUP, 4, 8, 2 * TOK), F32),
            pltpu.VMEM((2, 4, EXP * PAIR, 2 * TOK), BF),
            pltpu.VMEM((2, 4, 2 * TOK, EXP * PAIR), BF),
            pltpu.VMEM((2, 4, EXP * PAIR, 128), F32),
            pltpu.VMEM((EXP, ROWS, 2 * FFN), BF),
            pltpu.VMEM((EXP, ROWS, FFN), F32),
            pltpu.VMEM((4, EXP, PAIR, DIM), BF),
            pltpu.VMEM((2, NK, 4, TOK, KC), F32),
            pltpu.VMEM((2, NK, 4, TOK, KC), F32),
            pltpu.VMEM((2, NK, 4, TOK, KC), F32),
            pltpu.VMEM((NK, 4, TOK, KC), F32),
            dma((6,)),
            dma((9,)),
            dma((8,)),
            dma((8,)),
            dma((3, 8)),
            dma((3, 8)),
            dma((NK, 8)),
            dma((NK, 8)),
            dma((2, NK)),
            dma((2, NK)),
            dma((NK, 4)),
            dma((NK, 4)),
        ],
        compiler_params=pltpu.CompilerParams(collective_id=0, has_side_effects=True, vmem_limit_bytes=K1_VMEM * 2**20),
        cost_estimate=pl.CostEstimate(flops=10**10, bytes_accessed=40 * 2**20, transcendentals=0),
    )(*[pltpu.with_memory_space_constraint(a, pltpu.HBM) for a in args])


K1_VMEM = 46
RELAYED = 0
TR = 256
MB = 512
SLOTS = 5


def weight_grad_kernel(u2, z2, h2, ab2, u1, z1, h1, ab1, g2, p2, d2, g1, p1, d1, g_buf, p_buf, d_buf, sem):
    flying = {}
    step = 0
    for u, z, h, ab, g_o, p_o, d_o in ((u2, z2, h2, ab2, g2, p2, d2), (u1, z1, h1, ab1, g1, p1, d1)):
        for e in range(EXP):
            slot = step % SLOTS
            for c in flying.pop(step - SLOTS, []):
                c.wait()
            mine = flying.setdefault(step, [])

            def write(buf, out, m, n):
                part = pl.ds(m * MB, MB)
                c = pltpu.make_async_copy(buf.at[slot, part], out.at[e, part], sem.at[slot, n])
                c.start()
                mine.append(c)

            for m in range(DIM // MB):
                span = slice(m * MB, (m + 1) * MB)
                both = dot(u[e, :, span], ab[e], TN)
                g_buf[slot, span, :] = both[:, :FFN]
                p_buf[slot, span, :] = both[:, FFN:]
                write(g_buf, g_o, m, m)
                write(p_buf, p_o, m, DIM // MB + m)
            for m in range(FFN // MB):
                span = slice(m * MB, (m + 1) * MB)
                d_buf[slot, span, :] = dot(h[e, :, span], z[e], TN)
                write(d_buf, d_o, m, 2 * (DIM // MB) + m)
            step += 1
    for cs in flying.values():
        for c in cs:
            c.wait()


def weight_grads(*rows):
    up = jax.ShapeDtypeStruct((EXP, DIM, FFN), F32)
    shapes = [up, up, jax.ShapeDtypeStruct((EXP, FFN, DIM), F32)] * 2
    return pl.pallas_call(
        weight_grad_kernel,
        in_specs=[pl.BlockSpec(memory_space=pltpu.VMEM)] * 8,
        out_specs=[pl.BlockSpec(memory_space=pl.ANY)] * 6,
        out_shape=shapes,
        scratch_shapes=[
            pltpu.VMEM((SLOTS, DIM, FFN), F32),
            pltpu.VMEM((SLOTS, DIM, FFN), F32),
            pltpu.VMEM((SLOTS, FFN, DIM), F32),
            pltpu.SemaphoreType.DMA((SLOTS, 2 * (DIM // MB) + FFN // MB)),
        ],
        compiler_params=pltpu.CompilerParams(vmem_limit_bytes=K2_VMEM * 2**20),
        cost_estimate=pl.CostEstimate(flops=6 * 10**9, bytes_accessed=62 * 2**20, transcendentals=0),
    )(*[pltpu.with_memory_space_constraint(r, pltpu.VMEM) for r in rows])


K2_VMEM = 36


def solution(mesh):
    tok_spec = P(("data", "expert"), None)
    weight_spec = P("expert", None, None)
    grad_spec = P(("data", "expert"), None, None)

    def local_step(x_tokens, y_mid, dy_out, experts_one, gates_one, slots_one, experts_two, gates_two, slots_two, w_gate_one, w_up_one, w_down_one, w_gate_two, w_up_two, w_down_two):
        res = exchange(
            y_mid, dy_out, x_tokens, experts_two.T, gates_two.T, slots_two.T, experts_one.T, gates_one.T, slots_one.T,
            w_gate_two, w_up_two, w_down_two, w_gate_one, w_up_one, w_down_one,
        )
        part, mid = res[8:12], res[12]
        back = [lax.ppermute(part[p], "expert", [(i, i ^ (2 * p)) for i in range(GROUP)]) for p in (1, 2, 3)]
        grads = weight_grads(*res[:8])
        total = part[0] + back[0] + back[1] + back[2]
        dx = (mid.astype(F32) + total).astype(BF)
        return (dx, grads[3], grads[4], grads[5], grads[0], grads[1], grads[2])

    return jax.shard_map(local_step, mesh=mesh, in_specs=(tok_spec,) * 9 + (weight_spec,) * 6, out_specs=(tok_spec,) + (grad_spec,) * 6, check_vma=False)
```
